256 devices in a mesh: section: 4 (over y), seq: 64 (over z, x, core).
Axes of the slice: x: 4, y: 4, z: 8, core: 2. Of those that a mesh axis runs over, the one named last changes fastest.
Arguments:
- patches: bfloat16 [64, 729, 1152], P('seq'), may hold values from -40 to 40
- fc_gain: float32 [4, 1152], P('section'), may hold values from 0.1 to 1.9
- fc_in: bfloat16 [4, 1152, 2176], P('section', 'seq'), may hold values from -0.1875 to 0.1875
- fc_in_bias: float32 [4, 2176], P('section'), may hold values from -3 to 3
- fc_out: bfloat16 [4, 2176, 1152], P('section', None, 'seq'), may hold values from -0.125 to 0.125
- fc_out_bias: float32 [4, 1152], P('section'), may hold values from -3 to 3
- proj_weight: bfloat16 [1152, 3584], P('seq'), may hold values from -0.1875 to 0.1875
- text_embed: bfloat16 [8192, 3584], P('seq'), may hold values from -40 to 40
- frame_start: int32 [64], replicated, may hold values from 0 to 8191, as said below
- frame_count: int32 [64], replicated, may hold values from 1 to 196, as said below
- segment_ids: int32 [8192], replicated, may hold values from 0 to 2, as said below
- norm_gain: float32 [3584], replicated, may hold values from 0.1 to 1.9
- query_weight: bfloat16 [3584, 2048], P(None, 'section'), may hold values from -3 to 3
- query_bias: float32 [2048], P('section'), may hold values from -3 to 3
- key_weight: bfloat16 [3584, 512], P(None, 'section'), may hold values from -1 to 1
- value_weight: bfloat16 [3584, 512], P(None, 'section'), may hold values from -0.09375 to 0.09375
- value_bias: float32 [512], P('section'), may hold values from -3 to 3
Outputs:
- attended: bfloat16 [8192, 2048], P('seq', 'section')
The draws below stay inside these ranges and needn't reach their ends.
Inputs may be any that keep to these rules, and one draw needn't show every extreme that they name: Frame f keeps its first frame_count[f] pooled tokens and places them at positions frame_start[f] to frame_start[f] + frame_count[f] - 1; frame f begins in shard f, at a position from f * 128 to (f + 1) * 128 - 1; every frame ends before the next one begins, and the last ends by position 8191. The frame of shard 64 / 2 - 1 runs into the next shard. `frame_count`: some frame keeps all 196 tokens. `segment_ids`: segment numbers never fall along the sequence, and each of 0, 1 and 2 occurs.
All inputs are finite; a program needn't handle non-finite values.
Results may differ from the reference program's by a relative error of at most 0.02.
Values may be sent and summed in bfloat16 or wider, within the bound.
A program may use at most 128 MiB of HBM per device.

```python
import math
import jax
import jax.numpy as jnp
from jax import lax

D = 1152
FF = 2176
GRID = 27
HM = 3584
HEAD = 128
KV_HEADS = 4
QPK = 4
L_DEV = 128
PATCH = 729
POOLED = 196
QHEADS = 16
LAYERS = 4
FRAMES = 64
L_TOTAL = 8192
N_SEQ = 64


def rough_field(key, lead_shape, feature_width):
    k_base, k_rows, k_cols = jax.random.split(key, 3)
    base_draw = jax.random.normal(k_base, lead_shape + (feature_width,), jnp.float32)
    base_draw = jnp.clip(base_draw, -4.0, 4.0)
    row_scale = jnp.exp(jax.random.uniform(k_rows, lead_shape + (1,), jnp.float32, -1.15, 1.15))
    col_scale = jnp.exp(jax.random.uniform(k_cols, (feature_width,), jnp.float32, -1.15, 1.15))
    return base_draw * row_scale * col_scale


def draw_patches(key, part):
    return rough_field(jax.random.fold_in(key, 3), (FRAMES, PATCH), D).astype(jnp.bfloat16)


def draw_text_embed(key, part):
    return rough_field(jax.random.fold_in(key, 4), (L_TOTAL,), HM).astype(jnp.bfloat16)


def attention_pair(key):
    k_keys, k_noise = jax.random.split(jax.random.fold_in(key, 7), 2)
    root_width = math.sqrt(HM)
    key_draw = jnp.clip(jax.random.normal(k_keys, (HM, KV_HEADS, 1, HEAD), jnp.float32), -6.0, 6.0) / root_width
    noise_draw = jnp.clip(jax.random.normal(k_noise, (HM, KV_HEADS, QPK, HEAD), jnp.float32), -6.0, 6.0) * (3.5 / root_width)
    queries = noise_draw
    queries = jnp.clip(queries, -3.0, 3.0).reshape(HM, KV_HEADS * QPK * HEAD)
    return (key_draw.reshape(HM, KV_HEADS * HEAD), queries)


def draw_query_weight(key, part):
    return attention_pair(key)[1].astype(jnp.bfloat16)


def draw_key_weight(key, part):
    return attention_pair(key)[0].astype(jnp.bfloat16)


def frame_layout(key):
    k_offsets, k_chosen, k_counts = jax.random.split(jax.random.fold_in(key, 13), 3)
    middle = FRAMES // 2 - 1
    offsets = jax.random.randint(k_offsets, (FRAMES,), 0, L_DEV)
    chosen = jax.random.randint(k_chosen, (), 0, FRAMES - 4)
    chosen = jnp.where(chosen >= middle - 1, chosen + 3, chosen)
    frame_index = jnp.arange(FRAMES)
    offsets = jnp.where(frame_index == chosen, 0, offsets)
    offsets = jnp.where(frame_index == chosen + 1, max(POOLED - L_DEV, 0), offsets)
    offsets = jnp.where((frame_index == middle) | (frame_index == middle + 1), L_DEV - 1, offsets)
    following = jnp.concatenate([offsets[1:], jnp.zeros((1,), offsets.dtype)])
    upper_limit = jnp.minimum(POOLED, L_DEV + following - offsets)
    upper_limit = jnp.where(frame_index == FRAMES - 1, jnp.minimum(POOLED, L_DEV - offsets), upper_limit)
    lower_limit = jnp.maximum(1, upper_limit // 2)
    counts = jax.random.randint(k_counts, (FRAMES,), lower_limit, upper_limit + 1)
    counts = jnp.where(frame_index == chosen, POOLED, counts)
    counts = jnp.where(frame_index == middle, upper_limit, counts)
    starts = frame_index * L_DEV + offsets
    return (starts.astype(jnp.int32), counts.astype(jnp.int32))


def draw_frame_start(key, part):
    return frame_layout(key)[0]


def draw_frame_count(key, part):
    return frame_layout(key)[1]


def draw_segment_ids(key, part):
    k_first, k_second = jax.random.split(jax.random.fold_in(key, 5))
    first_cut = jax.random.randint(k_first, (), L_TOTAL // 16, L_TOTAL // 8)
    second_cut = jax.random.randint(k_second, (), L_TOTAL // 8, L_TOTAL // 4)
    positions = jnp.arange(L_TOTAL)
    return ((positions >= first_cut).astype(jnp.int32) + (positions >= second_cut).astype(jnp.int32)).astype(jnp.int32)


def block_levels(own_key, dims, cuts, least, largest):
    def one(position, parts):
        draws = jax.random.uniform(jax.random.fold_in(jax.random.fold_in(own_key, 6), position), (parts,), jnp.float32, least / len(cuts), largest / len(cuts))
        return jnp.repeat(jnp.exp(draws), dims[position] // parts).reshape((-1,) + (1,) * (len(dims) - position - 1))

    gain = one(*cuts[0])
    for cut in cuts[1:]:
        gain = gain * one(*cut)
    return gain


def noise(rng, dims, deviation, reach, pieces=(), kind=jnp.bfloat16):
    gain = block_levels(rng, dims, pieces, -0.22, 0.18) if pieces else 1.0
    array = jax.random.normal(rng, dims, jnp.float32) * deviation * gain
    return jnp.minimum(jnp.maximum(array, -reach), reach).astype(kind)


def setup_inputs(seed: int = 0) -> dict:
    arg_keys = jax.random.split(jax.random.key(seed), 18)
    patches = draw_patches(jax.random.fold_in(arg_keys[17], 71), 0)
    fc_gain = jnp.clip(1.0 + 0.18 * jax.random.normal(arg_keys[1], (LAYERS, D), jnp.float32), 0.1, 1.9)
    fc_in = noise(arg_keys[2], (LAYERS, D, FF), D ** -0.5, 0.1875, ((0, 4), (1, 64)))
    fc_in_bias = noise(arg_keys[3], (LAYERS, FF), 0.5, 3.0, ((0, 4),), jnp.float32)
    fc_out = noise(arg_keys[4], (LAYERS, FF, D), FF ** -0.5, 0.125, ((0, 4), (2, 64)))
    fc_out_bias = noise(arg_keys[5], (LAYERS, D), 0.5, 3.0, ((0, 4),), jnp.float32)
    proj_weight = noise(arg_keys[6], (D, HM), D ** -0.5, 0.1875, ((0, 64),))
    text_embed = draw_text_embed(jax.random.fold_in(arg_keys[17], 71), 0)
    frame_start = draw_frame_start(jax.random.fold_in(arg_keys[17], 71), 0)
    frame_count = draw_frame_count(jax.random.fold_in(arg_keys[17], 71), 0)
    segment_ids = draw_segment_ids(jax.random.fold_in(arg_keys[17], 71), 0)
    norm_gain = jnp.clip(1.0 + 0.18 * jax.random.normal(arg_keys[11], (HM,), jnp.float32), 0.1, 1.9)
    query_weight = draw_query_weight(jax.random.fold_in(arg_keys[17], 71), 0)
    query_bias = noise(arg_keys[13], (QHEADS * HEAD,), 0.5, 3.0, ((0, 4),), jnp.float32)
    key_weight = draw_key_weight(jax.random.fold_in(arg_keys[17], 71), 0)
    value_weight = noise(arg_keys[15], (HM, KV_HEADS * HEAD), HM ** -0.5, 0.09375, ((1, 4),))
    value_bias = noise(arg_keys[16], (KV_HEADS * HEAD,), 0.5, 3.0, ((0, 4),), jnp.float32)
    return {"patches": patches, "fc_gain": fc_gain, "fc_in": fc_in, "fc_in_bias": fc_in_bias, "fc_out": fc_out, "fc_out_bias": fc_out_bias, "proj_weight": proj_weight, "text_embed": text_embed, "frame_start": frame_start, "frame_count": frame_count, "segment_ids": segment_ids, "norm_gain": norm_gain, "query_weight": query_weight, "query_bias": query_bias, "key_weight": key_weight, "value_weight": value_weight, "value_bias": value_bias}


layer_eps = 1e-06
rms_eps = 1e-06
rope_base = 1000000.0

def layer_norm(values, scales):
    widened = values.astype(jnp.float32)
    center = widened - lax.optimization_barrier(jnp.mean(widened, axis=-1, keepdims=True))
    spread = lax.optimization_barrier(jnp.mean(center * center, axis=-1, keepdims=True))
    return center * lax.rsqrt(spread + layer_eps) * scales

def encoder_layer(values, scales, w_in, b_in, w_out, b_out):
    normed = layer_norm(values, scales).astype(jnp.bfloat16)
    hidden = jax.nn.gelu(jnp.dot(normed, w_in, preferred_element_type=jnp.float32) + b_in, approximate=True).astype(jnp.bfloat16)
    summed = values.astype(jnp.float32) + jnp.dot(hidden, w_out, preferred_element_type=jnp.float32) + b_out
    return summed.astype(jnp.bfloat16)

def pool_frame(encoded):
    lead_dims = encoded.shape[:-2]
    channel = encoded.shape[-1]
    grid_side = GRID
    pool_side = (GRID + 1) // 2
    grid_cells = encoded.astype(jnp.float32).reshape(lead_dims + (grid_side, grid_side, channel))
    pad_cells = 2 * pool_side - grid_side
    grid_cells = jnp.pad(grid_cells, [(0, 0)] * len(lead_dims) + [(0, pad_cells), (0, pad_cells), (0, 0)])
    totals = grid_cells.reshape(lead_dims + (pool_side, 2, pool_side, 2, channel)).sum(axis=(-4, -2))
    counts = jnp.minimum(2, grid_side - 2 * jnp.arange(pool_side)).astype(jnp.float32)
    cell_area = counts[:, None] * counts[None, :]
    return (totals / cell_area[..., None]).reshape(lead_dims + (pool_side * pool_side, channel))

def rotate(values, positions):
    head_dim = values.shape[-1]
    half_dim = head_dim // 2
    inv_rates = jnp.exp(jnp.arange(half_dim, dtype=jnp.float32) * (-2.0 * math.log(rope_base) / head_dim))
    angles = positions.astype(jnp.float32)[:, None] * inv_rates[None, :]
    cosine = jnp.cos(angles)[:, None, :]
    sine_part = jnp.sin(angles)[:, None, :]
    first_half = values[..., :half_dim]
    second = values[..., half_dim:]
    return jnp.concatenate([first_half * cosine - second * sine_part, second * cosine + first_half * sine_part], axis=-1)

def reference(patches, fc_gain, fc_in, fc_in_bias, fc_out, fc_out_bias, proj_weight, text_embed, frame_start, frame_count, segment_ids, norm_gain, query_weight, query_bias, key_weight, value_weight, value_bias):
    encoded = patches.reshape(FRAMES * PATCH, D)
    for layer_index in range(LAYERS):
        encoded = encoder_layer(encoded, fc_gain[layer_index], fc_in[layer_index], fc_in_bias[layer_index], fc_out[layer_index], fc_out_bias[layer_index])
    pooled = pool_frame(encoded.reshape(FRAMES, PATCH, D)).astype(jnp.bfloat16)
    projected = jnp.dot(pooled.reshape(FRAMES * POOLED, D), proj_weight, preferred_element_type=jnp.float32).astype(jnp.bfloat16)
    positions = jnp.arange(L_TOTAL, dtype=jnp.int32)
    home_frame = (positions // L_DEV).astype(jnp.int32)
    before = jnp.maximum(home_frame - 1, 0).astype(jnp.int32)

    def pick_tokens(frame_ids, ok_extra):
        offset = positions - frame_start[frame_ids]
        is_valid = ok_extra & (offset >= 0) & (offset < frame_count[frame_ids])
        picked = jnp.take(projected, frame_ids * POOLED + jnp.clip(offset, 0, POOLED - 1), axis=0)
        return (is_valid, picked)
    own_valid, own_rows = pick_tokens(home_frame, True)
    prev_valid, prev_rows = pick_tokens(before, home_frame > 0)
    inputs = jnp.where(own_valid[:, None], own_rows, jnp.where(prev_valid[:, None], prev_rows, text_embed))
    widened = inputs.astype(jnp.float32)
    normed = (widened * lax.rsqrt(lax.optimization_barrier(jnp.mean(widened * widened, axis=-1, keepdims=True)) + rms_eps) * norm_gain).astype(jnp.bfloat16)
    queries = jnp.dot(normed, query_weight, preferred_element_type=jnp.float32) + query_bias
    queries = rotate(queries.reshape(L_TOTAL, KV_HEADS * QPK, HEAD), positions).astype(jnp.bfloat16)
    key_heads = jnp.dot(normed, key_weight, preferred_element_type=jnp.float32)
    key_heads = rotate(key_heads.reshape(L_TOTAL, KV_HEADS, HEAD), positions).astype(jnp.bfloat16)
    values = (jnp.dot(normed, value_weight, preferred_element_type=jnp.float32) + value_bias).astype(jnp.bfloat16)
    values = values.reshape(L_TOTAL, KV_HEADS, HEAD)
    key_float = key_heads.astype(jnp.float32)
    value_float = values.astype(jnp.float32)
    score_scale = 1.0 / math.sqrt(HEAD)

    def attend_rows(block_index):
        row_start = (block_index * L_DEV).astype(jnp.int32)
        query_rows = lax.dynamic_slice_in_dim(queries, row_start, L_DEV, 0).astype(jnp.float32)
        query_rows = query_rows.reshape(L_DEV, KV_HEADS, QPK, HEAD)
        query_pos = row_start + jnp.arange(L_DEV, dtype=jnp.int32)
        query_seg = lax.dynamic_slice_in_dim(segment_ids, row_start, L_DEV, 0)
        scores = jnp.einsum('qgjd,kgd->gjqk', query_rows, key_float) * score_scale
        allowed = (positions[None, :] <= query_pos[:, None]) & (segment_ids[None, :] == query_seg[:, None])
        row_top = lax.optimization_barrier(jnp.max(jnp.where(allowed, scores, -jnp.inf), axis=-1, keepdims=True))
        weights = jnp.where(allowed, jnp.exp(scores - row_top), 0.0)
        row_total = lax.optimization_barrier(jnp.sum(weights, axis=-1))
        rounded = lax.optimization_barrier(weights.astype(jnp.bfloat16)).astype(jnp.float32)
        mixed = jnp.einsum('gjqk,kgd->qgjd', rounded, value_float)
        mixed = mixed / jnp.transpose(row_total, (2, 0, 1))[..., None]
        return mixed.reshape(L_DEV, KV_HEADS * QPK * HEAD).astype(jnp.bfloat16)
    attended = lax.map(attend_rows, jnp.arange(N_SEQ, dtype=jnp.int32))
    return attended.reshape(L_TOTAL, KV_HEADS * QPK * HEAD)
```

```python
import functools
import math

import jax
import jax.numpy as jnp
from jax import lax
from jax.experimental import pallas as pl
from jax.experimental.pallas import tpu as pltpu
from jax.sharding import PartitionSpec as P

NZ, NX, NC = 8, 4, 2


def seq_id(z, x, c):
    return lax.rem(z + NZ, NZ) * (NX * NC) + lax.rem(x + NX, NX) * NC + c


class Ring:
    def __init__(self, send_sem, recv_sem):
        self.send_sem, self.recv_sem, self.used, self.live = send_sem, recv_sem, 0, []

    def copy(self, sent, got, target):
        n = self.used
        self.used += 1
        out = pltpu.make_async_remote_copy(
            src_ref=sent, dst_ref=sent, send_sem=self.send_sem.at[n], recv_sem=self.recv_sem.at[n],
            device_id={"seq": target}, device_id_type=pl.DeviceIdType.MESH)
        into = pltpu.make_async_remote_copy(
            src_ref=got, dst_ref=got, send_sem=self.send_sem.at[n], recv_sem=self.recv_sem.at[n],
            device_id={"seq": target}, device_id_type=pl.DeviceIdType.MESH)
        self.live.append(out)
        return out, into

    def finish(self):
        for out in self.live:
            out.wait_send()


def greet(targets):
    barrier = pltpu.get_barrier_semaphore()
    for t in targets:
        pl.semaphore_signal(barrier, inc=1, device_id={"seq": t}, device_id_type=pl.DeviceIdType.MESH)
    pl.semaphore_wait(barrier, len(targets))


def torus_gather(ring, me, a_one, a_many, b_one, b_many):
    z, x, c = me
    s = 1 - 2 * c
    zm, zo = seq_id(z + s, x, c), seq_id(z - s, x, c)
    xm, xo = seq_id(z, x + s, c), seq_id(z, x - s, c)
    mate = seq_id(z, x, 1 - c)
    zw = lambda k: lax.rem(z + k + 2 * NZ, NZ)
    xw = lambda k: lax.rem(x + k + 2 * NX, NX)
    ax_m = [ring.copy(a_one(z, xw(-k * s)), a_one(z, xw(-(k + 1) * s)), xm) for k in range(2)]
    ax_o = ring.copy(a_one(z, x), a_one(z, xw(s)), xo)
    bz_m = [ring.copy(b_one(zw(-k * s), x), b_one(zw(-(k + 1) * s), x), zm) for k in range(4)]
    bz_o = [ring.copy(b_one(zw(k * s), x), b_one(zw((k + 1) * s), x), zo) for k in range(3)]
    az_m = [ring.copy(a_many(zw(-k * s), c), a_many(zw(-(k + 1) * s), c), zm) for k in range(4)]
    az_o = [ring.copy(a_many(zw(k * s), c), a_many(zw((k + 1) * s), c), zo) for k in range(3)]
    bx_m = [ring.copy(b_many(xw(-k * s), c), b_many(xw(-(k + 1) * s), c), xm) for k in range(2)]
    bx_o = ring.copy(b_many(x, c), b_many(xw(s), c), xo)
    mates = []

    def to_mate(sent, got):
        pair = ring.copy(sent, got, mate)
        pair[0].start()
        mates.append(pair)

    a_mate = lambda k: to_mate(a_many(zw(k * s), c), a_many(zw(-k * s), 1 - c))
    b_mate = lambda k: to_mate(b_many(xw(k * s), c), b_many(xw(-k * s), 1 - c))

    ax_m[0][0].start()
    ax_o[0].start()
    bz_m[0][0].start()
    bz_o[0][0].start()
    ax_m[0][1].wait_recv()
    ax_m[1][0].start()
    for k in range(3):
        bz_m[k][1].wait_recv()
        bz_m[k + 1][0].start()
        bz_o[k][1].wait_recv()
        if k < 2:
            bz_o[k + 1][0].start()
        if k == 1:
            ax_o[1].wait_recv()
            ax_m[1][1].wait_recv()
    az_m[0][0].start()
    az_o[0][0].start()
    a_mate(0)
    bz_m[3][1].wait_recv()
    bx_m[0][0].start()
    bx_o[0].start()
    b_mate(0)
    az_m[0][1].wait_recv()
    az_m[1][0].start()
    a_mate(-1)
    az_o[0][1].wait_recv()
    az_o[1][0].start()
    a_mate(1)
    bx_m[0][1].wait_recv()
    bx_m[1][0].start()
    b_mate(-1)
    az_m[1][1].wait_recv()
    az_m[2][0].start()
    a_mate(-2)
    az_o[1][1].wait_recv()
    az_o[2][0].start()
    a_mate(2)
    bx_o[1].wait_recv()
    b_mate(1)
    az_m[2][1].wait_recv()
    az_m[3][0].start()
    a_mate(-3)
    az_o[2][1].wait_recv()
    a_mate(3)
    bx_m[1][1].wait_recv()
    b_mate(-2)
    az_m[3][1].wait_recv()
    a_mate(-4)
    for pair in mates:
        pair[1].wait_recv()


GATHER_COPIES = 3 + 7 + 7 + 3 + 8 + 4


def kv_gather_kernel(kv_ref, a_ref, b_ref, send_sem, recv_sem, own_sem):
    me_seq = lax.axis_index("seq")
    z, x, c = me_seq // (NX * NC), lax.rem(me_seq // NC, NX), lax.rem(me_seq, NC)
    half = kv_ref.shape[0] // 2
    mine = [
        pltpu.make_async_copy(kv_ref.at[pl.ds(0, half)], a_ref.at[z, x, c], own_sem.at[0]),
        pltpu.make_async_copy(kv_ref.at[pl.ds(half, half)], b_ref.at[z, x, c], own_sem.at[1]),
    ]
    for copy in mine:
        copy.start()
    greet([seq_id(z + 1, x, c), seq_id(z - 1, x, c), seq_id(z, x + 1, c), seq_id(z, x - 1, c), seq_id(z, x, 1 - c)])
    for copy in mine:
        copy.wait()
    ring = Ring(send_sem, recv_sem)
    torus_gather(
        ring, (z, x, c),
        lambda zz, xx: a_ref.at[zz, xx, c], lambda zz, cc: a_ref.at[zz, :, cc],
        lambda zz, xx: b_ref.at[zz, xx, c], lambda xx, cc: b_ref.at[:, xx, cc])
    ring.finish()


def kv_gather(kv):
    half = kv.shape[0] // 2
    shape = jax.ShapeDtypeStruct((NZ, NX, NC, half, kv.shape[1]), kv.dtype)
    return pl.pallas_call(
        kv_gather_kernel,
        out_shape=(shape, shape),
        in_specs=[pl.BlockSpec(memory_space=pltpu.VMEM)],
        out_specs=(pl.BlockSpec(memory_space=pltpu.VMEM),) * 2,
        scratch_shapes=[
            pltpu.SemaphoreType.DMA((GATHER_COPIES,)),
            pltpu.SemaphoreType.DMA((GATHER_COPIES,)),
            pltpu.SemaphoreType.DMA((2,)),
        ],
        compiler_params=pltpu.CompilerParams(collective_id=1, has_side_effects=True, vmem_limit_bytes=40 << 20),
        cost_estimate=pl.CostEstimate(flops=0, bytes_accessed=40_000_000, transcendentals=0),
        name="kv_gather",
    )(kv)


def flash_kernel(info_ref, q_ref, a_ref, b_ref, qseg_ref, aseg_ref, bseg_ref, o_ref):
    shard = info_ref[0]
    own_z = shard // 8
    rows, head = q_ref.shape
    keys = a_ref.shape[1]
    half = keys // 8
    q = q_ref[...]
    qseg = qseg_ref[...]
    row = lax.rem(lax.broadcasted_iota(jnp.int32, (rows, 1), 0), 128)
    qpos = row + lax.rem(shard, 8) * 128
    col = lax.broadcasted_iota(jnp.int32, (1, keys), 1)
    kpos = (col // half) * 128 + lax.rem(col, half)
    scale = 1.0 / math.sqrt(head)

    def visit(carried, kv, kseg, extra):
        top, total, acc = carried
        s = lax.dot_general(q, kv[:, :head], (((1,), (1,)), ((), ())), preferred_element_type=jnp.float32)
        allowed = kseg == qseg
        if extra is not None:
            allowed = allowed & extra
        s = jnp.where(allowed, s * scale, -1e30)
        new_top = jnp.maximum(top, jnp.max(s, axis=1, keepdims=True))
        w = jnp.exp(s - new_top)
        if extra is not None:
            w = jnp.where(allowed, w, 0.0)
        keep = jnp.exp(top - new_top)
        total = total * keep + jnp.sum(w, axis=1, keepdims=True)
        acc = acc * keep + jnp.dot(w.astype(jnp.bfloat16), kv[:, head:], preferred_element_type=jnp.float32)
        return new_top, total, acc

    state = (
        jnp.full((rows, 1), -1e30, jnp.float32),
        jnp.zeros((rows, 1), jnp.float32),
        jnp.zeros((rows, head), jnp.float32),
    )
    state = visit(state, a_ref[own_z], aseg_ref[own_z], kpos <= qpos)
    state = visit(state, b_ref[own_z], bseg_ref[own_z], kpos + half <= qpos)

    def body(i, carried):
        z = own_z - 1 - i
        carried = visit(carried, a_ref[z], aseg_ref[z], None)
        return visit(carried, b_ref[z], bseg_ref[z], None)

    first_seg = info_ref[1]
    count = jnp.int32(0)
    for z in range(8):
        count = count + ((z < own_z) & (info_ref[2 + z] >= first_seg)).astype(jnp.int32)
    top, total, acc = lax.fori_loop(0, count, body, state)
    o_ref[...] = (acc / total).astype(o_ref.dtype)


def flash(q, a, b, segment_ids, shard, rows):
    a = a.reshape(8, -1, a.shape[-1])
    b = b.reshape(8, -1, b.shape[-1])
    halves = segment_ids.reshape(8, 8, 2, 64)
    aseg = halves[:, :, 0].reshape(8, 1, 512)
    bseg = halves[:, :, 1].reshape(8, 1, 512)
    own = lax.dynamic_slice_in_dim(segment_ids, shard * rows, rows, 0)
    qseg = jnp.tile(own, q.shape[0] // rows)[:, None]
    last = segment_ids.reshape(8, 1024)[:, -1]
    info = jnp.concatenate([shard[None].astype(jnp.int32), own[:1], last])
    whole = pl.BlockSpec(memory_space=pltpu.VMEM)
    return pl.pallas_call(
        flash_kernel,
        out_shape=jax.ShapeDtypeStruct(q.shape, jnp.bfloat16),
        in_specs=[pl.BlockSpec(memory_space=pltpu.SMEM)] + [whole] * 6,
        out_specs=whole,
        compiler_params=pltpu.CompilerParams(vmem_limit_bytes=48 << 20),
        cost_estimate=pl.CostEstimate(flops=2 * 10**9, bytes_accessed=5_000_000, transcendentals=4_000_000),
        name="flash",
    )(info, q, a, b, qseg, aseg, bseg)


GRID = 27


layer_eps = 1e-06
rms_eps = 1e-06
rope_base = 1000000.0
mask_floor = -1e30


def turned_gather(arrays, axis, dims):
    turned = [jnp.moveaxis(a, dim, 0) for a, dim in zip(arrays, dims)]
    both = jnp.concatenate([t.reshape(len(t), -1) for t in turned], axis=1)
    filled, at, finished = (lax.all_gather(both, axis, axis=0, tiled=True), 0, [])
    for t, dim in zip(turned, dims):
        section = filled[:, at : at + t[0].size].reshape(-1, *t.shape[1:])
        finished.append(jnp.moveaxis(section, 0, dim))
        at += t[0].size
    return tuple(finished)


def passed_along(block, axis, distance):
    devices = range(lax.axis_size(axis))
    route = [(i - distance, i) for i in devices if i - distance in devices]
    return lax.ppermute(block, axis, route)


def from_root(x, axis, root):
    return lax.dynamic_index_in_dim(lax.all_gather(x, axis), root, 0, keepdims=False)


def layer_norm(values, scales):
    widened = values.astype(jnp.float32)
    center = widened - jnp.mean(widened, axis=-1, keepdims=True)
    spread = jnp.mean(center * center, axis=-1, keepdims=True)
    return center * lax.rsqrt(spread + layer_eps) * scales


def encoder_layer(values, scales, w_in, b_in, w_out, b_out):
    normed = layer_norm(values, scales).astype(jnp.bfloat16)
    hidden = jax.nn.gelu(
        jnp.dot(normed, w_in, preferred_element_type=jnp.float32) + b_in, approximate=True
    ).astype(jnp.bfloat16)
    summed = (
        values.astype(jnp.float32)
        + jnp.dot(hidden, w_out, preferred_element_type=jnp.float32)
        + b_out
    )
    return summed.astype(jnp.bfloat16)


def pool_frame(encoded):
    channel = encoded.shape[-1]
    grid_side = GRID
    pool_side = (GRID + 1) // 2
    grid_cells = encoded.astype(jnp.float32).reshape(grid_side, grid_side, channel)
    pad_cells = 2 * pool_side - grid_side
    grid_cells = jnp.pad(grid_cells, [(0, pad_cells), (0, pad_cells), (0, 0)])
    totals = grid_cells.reshape(pool_side, 2, pool_side, 2, channel).sum(axis=(1, 3))
    counts = jnp.minimum(2, grid_side - 2 * jnp.arange(pool_side)).astype(jnp.float32)
    cell_area = counts[:, None] * counts[None, :]
    return (totals / cell_area[..., None]).reshape(pool_side * pool_side, channel)


def rotate(values, positions):
    head_dim = values.shape[-1]
    half_dim = head_dim // 2
    inv_rates = jnp.exp(
        jnp.arange(half_dim, dtype=jnp.float32) * (-2.0 * math.log(rope_base) / head_dim)
    )
    angles = positions.astype(jnp.float32)[:, None] * inv_rates[None, :]
    cosine = jnp.cos(angles)[:, None, :]
    sine_part = jnp.sin(angles)[:, None, :]
    first_half = values[..., :half_dim]
    second = values[..., half_dim:]
    return jnp.concatenate(
        [first_half * cosine - second * sine_part, second * cosine + first_half * sine_part],
        axis=-1,
    )


def take_rows(source, offsets, upper_limit):
    is_valid = (offsets >= 0) & (offsets < upper_limit)
    picked = jnp.take(source, jnp.clip(offsets, 0, source.shape[0] - 1), axis=0)
    return (jnp.where(is_valid[:, None], picked, jnp.zeros((), source.dtype)), is_valid)


def per_device(
    patches,
    fc_gain,
    fc_in,
    fc_in_bias,
    fc_out,
    fc_out_bias,
    proj_weight,
    text_embed,
    frame_start,
    frame_count,
    segment_ids,
    norm_gain,
    query_weight,
    query_bias,
    key_weight,
    value_weight,
    value_bias,
):
    section_count = lax.axis_size("section")
    section_id = lax.axis_index("section")
    shard_count = lax.axis_size("seq")
    shard_id = lax.axis_index("seq")
    shard_rows = text_embed.shape[0]
    model_width = text_embed.shape[1]
    head_size = key_weight.shape[1]
    group_size = query_weight.shape[1] // head_size
    frame_patches = patches[0]
    patch_rows, feature_width = frame_patches.shape
    column_count = model_width // section_count
    proj_block = lax.dynamic_slice_in_dim(proj_weight, section_id * column_count, column_count, 1)
    w_in, w_out, proj_full = turned_gather((fc_in, fc_out, proj_block), "seq", (1, 2, 0))
    w_in = w_in[0]
    w_out = w_out[0]
    layer_gain = fc_gain[0]
    bias_in = fc_in_bias[0]
    bias_out = fc_out_bias[0]
    band_rows = 9
    batch_rows = band_rows * GRID
    batches = GRID // band_rows
    tick_count = batches + section_count - 1
    first_section = section_id == 0
    last_section = section_id == section_count - 1

    def run_tick(tick_index, loop_carry):
        inflow, collected = loop_carry
        feed_rows = lax.dynamic_slice_in_dim(
            frame_patches, jnp.minimum(tick_index, batches - 1) * batch_rows, batch_rows, 0
        )
        result = encoder_layer(
            jnp.where(first_section, feed_rows, inflow), layer_gain, w_in, bias_in, w_out, bias_out
        )
        slot_start = jnp.clip(tick_index - section_count + 1, 0, batches - 1) * batch_rows
        current = lax.dynamic_slice_in_dim(collected, slot_start, batch_rows, 0)
        is_ready = last_section & (tick_index >= section_count - 1)
        collected = lax.dynamic_update_slice_in_dim(
            collected, jnp.where(is_ready, result, current), slot_start, 0
        )
        inflow = passed_along(result, "section", 1)
        return (inflow, collected)

    start_state = (
        jnp.zeros((batch_rows, feature_width), jnp.bfloat16),
        jnp.zeros((patch_rows, feature_width), jnp.bfloat16),
    )
    inflow, collected = lax.fori_loop(0, tick_count, run_tick, start_state)
    pooled = pool_frame(collected).astype(jnp.bfloat16)
    local_slots = jnp.arange(shard_rows, dtype=jnp.int32)
    positions = shard_id * shard_rows + local_slots
    own_start = frame_start[shard_id]
    own_count = frame_count[shard_id]
    previous = jnp.maximum(shard_id - 1, 0)
    prev_offsets = positions - frame_start[previous]
    prev_valid = (shard_id > 0) & (prev_offsets >= 0) & (prev_offsets < frame_count[previous])
    own_rows, own_valid = take_rows(pooled, positions - own_start, own_count)
    sent_rows, sent_valid = take_rows(pooled, positions + shard_rows - own_start, own_count)
    arrived = passed_along(sent_rows, "seq", 1)
    vision = jnp.where(own_valid[:, None], own_rows, arrived)
    vision = from_root(vision, "section", section_count - 1)
    block_cols = jnp.dot(vision, proj_full, preferred_element_type=jnp.float32).astype(jnp.bfloat16)
    text_cols = lax.dynamic_slice_in_dim(text_embed, section_id * column_count, column_count, 1)
    mixed_cols = jnp.where((own_valid | prev_valid)[:, None], block_cols, text_cols)
    inputs = lax.all_gather(mixed_cols, "section", axis=1, tiled=True)
    widened = inputs.astype(jnp.float32)
    normed = (
        widened
        * lax.rsqrt(jnp.mean(widened * widened, axis=1, keepdims=True) + rms_eps)
        * norm_gain
    ).astype(jnp.bfloat16)
    queries = jnp.dot(normed, query_weight, preferred_element_type=jnp.float32) + query_bias
    queries = rotate(queries.reshape(shard_rows, group_size, head_size), positions).astype(
        jnp.bfloat16
    )
    key_heads = jnp.dot(normed, key_weight, preferred_element_type=jnp.float32)
    key_heads = rotate(key_heads.reshape(shard_rows, 1, head_size), positions).astype(jnp.bfloat16)
    key_heads = key_heads.reshape(shard_rows, head_size)
    values = (
        jnp.dot(normed, value_weight, preferred_element_type=jnp.float32) + value_bias
    ).astype(jnp.bfloat16)
    stacked = jnp.concatenate([key_heads, values], axis=1)
    queries = queries.reshape(shard_rows, group_size, head_size).transpose(1, 0, 2)
    queries = queries.reshape(shard_rows * group_size, head_size)
    half_a, half_b = kv_gather(stacked)
    attended = flash(queries, half_a, half_b, segment_ids, shard_id, shard_rows)
    attended = attended.reshape(group_size, shard_rows, head_size).transpose(1, 0, 2)
    return attended.reshape(shard_rows, group_size * head_size)


def solution(mesh):
    return jax.shard_map(
        per_device,
        mesh=mesh,
        in_specs=(
            P("seq", None, None),
            P("section", None),
            P("section", "seq", None),
            P("section", None),
            P("section", None, "seq"),
            P("section", None),
            P("seq", None),
            P("seq", None),
            P(),
            P(),
            P(),
            P(),
            P(None, "section"),
            P("section"),
            P(None, "section"),
            P(None, "section"),
            P("section"),
        ),
        out_specs=P("seq", "section"),
        check_vma=False,
    )
```

```python
import functools
import math

import jax
import jax.numpy as jnp
from jax import lax
from jax.experimental import pallas as pl
from jax.experimental.pallas import tpu as pltpu
from jax.sharding import PartitionSpec as P

NZ, NX, NC = 8, 4, 2


def seq_id(z, x, c):
    return lax.rem(z + NZ, NZ) * (NX * NC) + lax.rem(x + NX, NX) * NC + c


class Ring:
    def __init__(self, send_sem, recv_sem):
        self.send_sem, self.recv_sem, self.used, self.live = send_sem, recv_sem, 0, []

    def copy(self, sent, got, target, into=None):
        n = self.used
        self.used += 1
        to = {"seq": target} if not isinstance(target, dict) else target
        sems = dict(send_sem=self.send_sem.at[n], recv_sem=self.recv_sem.at[n])
        make = functools.partial(
            pltpu.make_async_remote_copy, device_id=to, device_id_type=pl.DeviceIdType.MESH, **sems)
        out = make(src_ref=sent, dst_ref=sent if into is None else into)
        into = make(src_ref=got, dst_ref=got)
        self.live.append(out)
        return out, into

    def finish(self):
        for out in self.live:
            out.wait_send()


def greet(targets):
    barrier = pltpu.get_barrier_semaphore()
    for t in targets:
        t = {"seq": t} if not isinstance(t, dict) else t
        pl.semaphore_signal(barrier, inc=1, device_id=t, device_id_type=pl.DeviceIdType.MESH)
    pl.semaphore_wait(barrier, len(targets))


def torus_gather(ring, me, a_one, a_many, b_one, b_many):
    z, x, c = me
    s = 1 - 2 * c
    zm, zo = seq_id(z + s, x, c), seq_id(z - s, x, c)
    xm, xo = seq_id(z, x + s, c), seq_id(z, x - s, c)
    mate = seq_id(z, x, 1 - c)
    zw = lambda k: lax.rem(z + k + 2 * NZ, NZ)
    xw = lambda k: lax.rem(x + k + 2 * NX, NX)
    ax_m = [ring.copy(a_one(z, xw(-k * s)), a_one(z, xw(-(k + 1) * s)), xm) for k in range(2)]
    ax_o = ring.copy(a_one(z, x), a_one(z, xw(s)), xo)
    bz_m = [ring.copy(b_one(zw(-k * s), x), b_one(zw(-(k + 1) * s), x), zm) for k in range(4)]
    bz_o = [ring.copy(b_one(zw(k * s), x), b_one(zw((k + 1) * s), x), zo) for k in range(3)]
    az_m = [ring.copy(a_many(zw(-k * s), c), a_many(zw(-(k + 1) * s), c), zm) for k in range(4)]
    az_o = [ring.copy(a_many(zw(k * s), c), a_many(zw((k + 1) * s), c), zo) for k in range(3)]
    bx_m = [ring.copy(b_many(xw(-k * s), c), b_many(xw(-(k + 1) * s), c), xm) for k in range(2)]
    bx_o = ring.copy(b_many(x, c), b_many(xw(s), c), xo)
    am = {k: ring.copy(a_many(zw(k * s), c), a_many(zw(-k * s), 1 - c), mate) for k in range(-4, 4)}
    bm = {k: ring.copy(b_many(xw(k * s), c), b_many(xw(-k * s), 1 - c), mate) for k in range(-2, 2)}
    go = lambda *pairs: [pair[0].start for pair in pairs]
    on = lambda *pairs: [pair[1].wait_recv for pair in pairs]
    return [
        go(ax_m[0], ax_o, bz_m[0], bz_o[0]),
        on(ax_m[0]) + go(ax_m[1]) + on(bz_m[0]) + go(bz_m[1]) + on(bz_o[0]) + go(bz_o[1]),
        on(bz_m[1]) + go(bz_m[2]) + on(bz_o[1]) + go(bz_o[2]) + on(ax_o, ax_m[1]),
        on(bz_m[2]) + go(bz_m[3]) + on(bz_o[2]) + go(az_m[0], az_o[0], am[0]),
        on(bz_m[3]) + go(bx_m[0], bx_o, bm[0]),
        on(az_m[0]) + go(az_m[1], am[-1]) + on(az_o[0]) + go(az_o[1], am[1]),
        on(bx_m[0]) + go(bx_m[1], bm[-1]) + on(az_m[1]) + go(az_m[2], am[-2]) + on(az_o[1]) + go(az_o[2], am[2]),
        on(bx_o) + go(bm[1]) + on(az_m[2]) + go(az_m[3], am[-3]) + on(az_o[2]) + go(am[3]),
        on(bx_m[1]) + go(bm[-2]) + on(az_m[3]) + go(am[-4]),
        on(*am.values(), *bm.values()),
    ]


def run(stage):
    for step in stage:
        step()


GATHER_COPIES = 3 + 7 + 7 + 3 + 8 + 4


def kv_gather_kernel(kv_ref, a_ref, b_ref, send_sem, recv_sem, own_sem):
    me_seq = lax.axis_index("seq")
    z, x, c = me_seq // (NX * NC), lax.rem(me_seq // NC, NX), lax.rem(me_seq, NC)
    half = kv_ref.shape[0] // 2
    mine = [
        pltpu.make_async_copy(kv_ref.at[pl.ds(0, half)], a_ref.at[z, x, c], own_sem.at[0]),
        pltpu.make_async_copy(kv_ref.at[pl.ds(half, half)], b_ref.at[z, x, c], own_sem.at[1]),
    ]
    for copy in mine:
        copy.start()
    greet([seq_id(z + 1, x, c), seq_id(z - 1, x, c), seq_id(z, x + 1, c), seq_id(z, x - 1, c), seq_id(z, x, 1 - c)])
    for copy in mine:
        copy.wait()
    ring = Ring(send_sem, recv_sem)
    for stage in torus_gather(
        ring, (z, x, c),
        lambda zz, xx: a_ref.at[zz, xx, c], lambda zz, cc: a_ref.at[zz, :, cc],
        lambda zz, xx: b_ref.at[zz, xx, c], lambda xx, cc: b_ref.at[:, xx, cc]):
        run(stage)
    ring.finish()


def kv_gather(kv):
    half = kv.shape[0] // 2
    shape = jax.ShapeDtypeStruct((NZ, NX, NC, half, kv.shape[1]), kv.dtype)
    return pl.pallas_call(
        kv_gather_kernel,
        out_shape=(shape, shape),
        in_specs=[pl.BlockSpec(memory_space=pltpu.VMEM)],
        out_specs=(pl.BlockSpec(memory_space=pltpu.VMEM),) * 2,
        scratch_shapes=[
            pltpu.SemaphoreType.DMA((GATHER_COPIES,)),
            pltpu.SemaphoreType.DMA((GATHER_COPIES,)),
            pltpu.SemaphoreType.DMA((2,)),
        ],
        compiler_params=pltpu.CompilerParams(collective_id=1, has_side_effects=True, vmem_limit_bytes=40 << 20),
        cost_estimate=pl.CostEstimate(flops=0, bytes_accessed=40_000_000, transcendentals=0),
        name="kv_gather",
    )(kv)


def flash_kernel(info_ref, q_ref, a_ref, b_ref, qseg_ref, aseg_ref, bseg_ref, o_ref):
    shard = info_ref[0]
    own_z = shard // 8
    rows, head = q_ref.shape
    keys = a_ref.shape[1]
    half = keys // 8
    q = q_ref[...]
    qseg = qseg_ref[...]
    row = lax.rem(lax.broadcasted_iota(jnp.int32, (rows, 1), 0), 128)
    qpos = row + lax.rem(shard, 8) * 128
    col = lax.broadcasted_iota(jnp.int32, (1, keys), 1)
    kpos = (col // half) * 128 + lax.rem(col, half)
    scale = 1.0 / math.sqrt(head)

    def visit(carried, kv, kseg, extra):
        top, total, acc = carried
        s = lax.dot_general(q, kv[:, :head], (((1,), (1,)), ((), ())), preferred_element_type=jnp.float32)
        allowed = kseg == qseg
        if extra is not None:
            allowed = allowed & extra
        s = jnp.where(allowed, s * scale, -1e30)
        new_top = jnp.maximum(top, jnp.max(s, axis=1, keepdims=True))
        w = jnp.exp(s - new_top)
        if extra is not None:
            w = jnp.where(allowed, w, 0.0)
        keep = jnp.exp(top - new_top)
        total = total * keep + jnp.sum(w, axis=1, keepdims=True)
        acc = acc * keep + jnp.dot(w.astype(jnp.bfloat16), kv[:, head:], preferred_element_type=jnp.float32)
        return new_top, total, acc

    state = (
        jnp.full((rows, 1), -1e30, jnp.float32),
        jnp.zeros((rows, 1), jnp.float32),
        jnp.zeros((rows, head), jnp.float32),
    )
    state = visit(state, a_ref[own_z], aseg_ref[own_z], kpos <= qpos)
    state = visit(state, b_ref[own_z], bseg_ref[own_z], kpos + half <= qpos)

    def body(i, carried):
        z = own_z - 1 - i
        carried = visit(carried, a_ref[z], aseg_ref[z], None)
        return visit(carried, b_ref[z], bseg_ref[z], None)

    first_seg = info_ref[1]
    count = jnp.int32(0)
    for z in range(8):
        count = count + ((z < own_z) & (info_ref[2 + z] >= first_seg)).astype(jnp.int32)
    top, total, acc = lax.fori_loop(0, count, body, state)
    o_ref[...] = (acc / total).astype(o_ref.dtype)


def flash(q, a, b, segment_ids, shard, rows):
    a = a.reshape(8, -1, a.shape[-1])
    b = b.reshape(8, -1, b.shape[-1])
    halves = segment_ids.reshape(8, 8, 2, 64)
    aseg = halves[:, :, 0].reshape(8, 1, 512)
    bseg = halves[:, :, 1].reshape(8, 1, 512)
    own = lax.dynamic_slice_in_dim(segment_ids, shard * rows, rows, 0)
    qseg = jnp.tile(own, q.shape[0] // rows)[:, None]
    last = segment_ids.reshape(8, 1024)[:, -1]
    info = jnp.concatenate([shard[None].astype(jnp.int32), own[:1], last])
    whole = pl.BlockSpec(memory_space=pltpu.VMEM)
    return pl.pallas_call(
        flash_kernel,
        out_shape=jax.ShapeDtypeStruct(q.shape, jnp.bfloat16),
        in_specs=[pl.BlockSpec(memory_space=pltpu.SMEM)] + [whole] * 6,
        out_specs=whole,
        compiler_params=pltpu.CompilerParams(vmem_limit_bytes=48 << 20),
        cost_estimate=pl.CostEstimate(flops=2 * 10**9, bytes_accessed=5_000_000, transcendentals=4_000_000),
        name="flash",
    )(info, q, a, b, qseg, aseg, bseg)


CHUNKS, CHUNK = 8, 96
ENC_COPIES = 7 + 7 + 2 * GATHER_COPIES + 8 + 1 + 6
layer_eps = 1e-06
rms_eps = 1e-06
rope_base = 1000000.0


def encoder_kernel(
    w_ref, p_ref, pick_ref, patches_ref, gain_ref, bin_ref, bout_ref, select_ref, text_ref, valid_ref,
    mixed_ref,
    rec_w, rec_p, win, wout, extra, pa, pb, inflow, outflow, passed, vision, acc,
    send_sem, recv_sem, chunk_send, chunk_recv, local_sem,
):
    me_seq, section = lax.axis_index("seq"), lax.axis_index("section")
    z, x, c = me_seq // (NX * NC), lax.rem(me_seq // NC, NX), lax.rem(me_seq, NC)
    j = lax.rem(me_seq, NX * NC)
    last = section == 3
    up, down = lax.rem(section + 1, 4), lax.rem(section + 3, 4)
    shards = NZ * NX * NC
    ahead, behind = lax.rem(me_seq + 1, shards), lax.rem(me_seq + shards - 1, shards)
    others = [lax.rem(j + k, 8) for k in range(8)]
    sources = [lax.rem(j + 8 - k, 8) for k in range(8)]
    member = lambda k: z * (NX * NC) + k

    own = [
        pltpu.make_async_copy(w_ref.at[j], rec_w.at[j], local_sem.at[0]),
        pltpu.make_async_copy(p_ref.at[j], rec_p.at[j], local_sem.at[1]),
    ]
    frame = pltpu.make_async_copy(patches_ref, inflow, local_sem.at[2])
    for copy in own:
        copy.start()

    @pl.when(section == 0)
    def _():
        frame.start()

    greet(
        [member(k) for k in others[1:]]
        + [seq_id(z + 1, x, c), seq_id(z - 1, x, c), ahead, behind, {"section": up}, {"section": down}]
    )
    ring = Ring(send_sem, recv_sem)
    spread_w = [ring.copy(w_ref.at[others[k]], rec_w.at[sources[k]], member(others[k]), rec_w.at[j]) for k in range(1, 8)]
    spread_p = [ring.copy(p_ref.at[others[k]], rec_p.at[sources[k]], member(others[k]), rec_p.at[j]) for k in range(1, 8)]
    for out, _ in spread_w:
        out.start()
    for copy in own:
        copy.wait()
    for _, into in spread_w:
        into.wait_recv()
    rows = win.shape[3]
    block = jnp.dot(pick_ref[...], rec_w[...].reshape(-1, rec_w.shape[2]), preferred_element_type=jnp.float32)
    block = block.astype(jnp.bfloat16)
    wout[x, c, z] = block[:, 256:512]
    win[x, c, z] = block[:, :256]
    extra[c, z] = block[:, 512:]

    def views(a, b):
        return (
            lambda zz, xx: a.at[xx, c, zz], lambda zz, cc: a.at[:, cc, zz],
            lambda zz, xx: b.at[xx, c, zz], lambda xx, cc: b.at[xx, cc])

    stages = torus_gather(ring, (z, x, c), *views(win, wout))
    s = 1 - 2 * c
    zw = lambda k: lax.rem(z + k + 2 * NZ, NZ)
    zm, zo = seq_id(z + s, x, c), seq_id(z - s, x, c)
    ez_m = [ring.copy(extra.at[c, zw(-k * s)], extra.at[c, zw(-(k + 1) * s)], zm) for k in range(4)]
    ez_o = [ring.copy(extra.at[c, zw(k * s)], extra.at[c, zw((k + 1) * s)], zo) for k in range(3)]
    e_mate = ring.copy(extra.at[c], extra.at[1 - c], seq_id(z, x, 1 - c))
    for n, stage in enumerate(stages):
        if n == 9:
            e_mate[0].start()
        run(stage)
        if n == 3:
            ez_m[0][0].start()
            ez_o[0][0].start()
        if 5 <= n < 9:
            ez_m[n - 5][1].wait_recv()
            if n < 8:
                ez_m[n - 4][0].start()
                ez_o[n - 5][1].wait_recv()
            if n < 7:
                ez_o[n - 4][0].start()
    e_mate[1].wait_recv()
    for out, _ in spread_p:
        out.start()

    def lay_out_p():
        for _, into in spread_p:
            into.wait_recv()
        block = jnp.dot(pick_ref[...], rec_p[...].reshape(-1, rec_p.shape[2]), preferred_element_type=jnp.float32)
        block = block.astype(jnp.bfloat16)
        pa[x, c, z] = block[:, :256]
        pb[x, c, z] = block[:, 256:]

    p_stages = [[lay_out_p]] + torus_gather(ring, (z, x, c), *views(pa, pb))

    @pl.when(last)
    def _():
        for stage in p_stages:
            run(stage)

    @pl.when(section == 0)
    def _():
        frame.wait()

    def chunk_copy(i):
        return pltpu.make_async_remote_copy(
            src_ref=outflow.at[i], dst_ref=inflow.at[i], send_sem=chunk_send.at[i], recv_sem=chunk_recv.at[i],
            device_id={"section": up}, device_id_type=pl.DeviceIdType.MESH)

    def one_chunk(i, nothing):
        @pl.when(section > 0)
        def _():
            chunk_copy(i).wait_recv()

        widened = inflow[i].astype(jnp.float32)
        center = widened - jnp.mean(widened, axis=1, keepdims=True)
        spread = jnp.mean(center * center, axis=1, keepdims=True)
        normed = (center * lax.rsqrt(spread + layer_eps) * gain_ref[...]).astype(jnp.bfloat16)
        acc[...] = widened + bout_ref[...]

        def part(w_in, b_in, w_out):
            v = jnp.dot(normed, w_in, preferred_element_type=jnp.float32) + b_in
            hidden = jax.nn.gelu(v, approximate=True).astype(jnp.bfloat16)
            return lax.dot_general(hidden, w_out, (((1,), (1,)), ((), ())), preferred_element_type=jnp.float32)

        for k in range(8):
            flat = lambda ref: ref[k // 2, k % 2].reshape(8 * rows, 256)
            acc[...] += part(flat(win), bin_ref[:, 256 * k : 256 * k + 256], flat(wout))
        acc[...] += part(extra[0].reshape(8 * rows, 128), bin_ref[:, 2048:], extra[1].reshape(8 * rows, 128))
        outflow[i] = acc[...].astype(jnp.bfloat16)

        @pl.when(jnp.logical_not(last))
        def _():
            chunk_copy(i).start()

        for n, stage in enumerate(p_stages[:CHUNKS]):
            @pl.when((i == n) & jnp.logical_not(last))
            def _():
                run(stage)

        return nothing

    lax.fori_loop(0, CHUNKS, one_chunk, 0)

    @pl.when(jnp.logical_not(last))
    def _():
        for stage in p_stages[CHUNKS:]:
            run(stage)
        for i in range(CHUNKS):
            chunk_copy(i).wait_send()

    half = vision.shape[2]
    over = pltpu.make_async_remote_copy(
        src_ref=passed.at[0], dst_ref=passed.at[1], send_sem=local_sem.at[3], recv_sem=local_sem.at[4],
        device_id={"seq": ahead}, device_id_type=pl.DeviceIdType.MESH)
    cast = lambda h, n, to: pltpu.make_async_remote_copy(
        src_ref=vision.at[h], dst_ref=vision.at[h], send_sem=local_sem.at[5 + n], recv_sem=local_sem.at[9 + h],
        device_id={"section": to}, device_id_type=pl.DeviceIdType.MESH)

    @pl.when(last)
    def _():
        encoded = outflow[...].reshape(CHUNKS * CHUNK, outflow.shape[2])
        count = select_ref.shape[0] // 2
        passed[0] = jnp.dot(select_ref[count:], encoded, preferred_element_type=jnp.float32).astype(jnp.bfloat16)
        over.start()
        mine = jnp.dot(select_ref[:count], encoded, preferred_element_type=jnp.float32)
        over.wait()
        mine = mine + jnp.where(me_seq > 0, passed[1].astype(jnp.float32), 0.0)
        mine = mine.astype(jnp.bfloat16)
        vision[0] = mine[:, :half]
        vision[1] = mine[:, half:]
        copies = [cast(0, 0, 0), cast(1, 1, 2), cast(1, 2, 0), cast(0, 3, 2)]
        for copy in copies:
            copy.start()
        for copy in copies:
            copy.wait_send()

    for me, first in ((0, 0), (2, 1)):
        @pl.when(section == me)
        def _():
            cast(first, 0, 1).wait_recv()
            on = cast(first, 0, 1)
            on.start()
            cast(1 - first, 0, 1).wait_recv()
            on.wait_send()

    @pl.when(section == 1)
    def _():
        cast(0, 0, 1).wait_recv()
        cast(1, 0, 1).wait_recv()

    left, right = vision[0], vision[1]
    valid = valid_ref[...] > 0
    for k in range(7):
        for n, ref in enumerate((pa, pb)):
            w = ref[k // 2, k % 2].reshape(8 * rows, 256)
            out = jnp.dot(left, w[:half], preferred_element_type=jnp.float32)
            out = out + jnp.dot(right, w[half:], preferred_element_type=jnp.float32)
            at = 512 * k + 256 * n
            mixed_ref[:, at : at + 256] = jnp.where(
                valid, out.astype(jnp.bfloat16), text_ref[:, at : at + 256])
    ring.finish()


def encode(w, p, patches, gain, b_in, b_out, select, text, valid):
    rows, width = w.shape[1] and 144, patches.shape[2]
    at = jnp.arange(rows)[:, None]
    pick = (jnp.arange(256)[None, :] == 32 * (at // 18) + at % 18).astype(jnp.bfloat16)
    whole = pl.BlockSpec(memory_space=pltpu.VMEM)
    bf = jnp.bfloat16
    big = pltpu.VMEM((NX, NC, NZ, rows, 256), bf)
    return pl.pallas_call(
        encoder_kernel,
        out_shape=jax.ShapeDtypeStruct(text.shape, bf),
        in_specs=[whole, whole, whole, pl.BlockSpec(memory_space=pl.ANY)] + [whole] * 6,
        out_specs=whole,
        scratch_shapes=[
            pltpu.VMEM(w.shape, bf), pltpu.VMEM(p.shape, bf),
            big, big, pltpu.VMEM((NC, NZ, rows, 128), bf), big, big,
            pltpu.VMEM((CHUNKS, CHUNK, width), bf), pltpu.VMEM((CHUNKS, CHUNK, width), bf),
            pltpu.VMEM((2, text.shape[0], width), bf), pltpu.VMEM((2, text.shape[0], width // 2), bf),
            pltpu.VMEM((CHUNK, width), jnp.float32),
            pltpu.SemaphoreType.DMA((ENC_COPIES,)), pltpu.SemaphoreType.DMA((ENC_COPIES,)),
            pltpu.SemaphoreType.DMA((CHUNKS,)), pltpu.SemaphoreType.DMA((CHUNKS,)),
            pltpu.SemaphoreType.DMA((12,)),
        ],
        compiler_params=pltpu.CompilerParams(collective_id=0, has_side_effects=True, vmem_limit_bytes=60 << 20),
        cost_estimate=pl.CostEstimate(flops=10**10, bytes_accessed=40_000_000, transcendentals=2_000_000),
        name="encode",
    )(w, p, pick, patches, gain, b_in, b_out, select, text, valid)


def rotate(values, positions):
    head_dim = values.shape[-1]
    half_dim = head_dim // 2
    inv_rates = jnp.exp(
        jnp.arange(half_dim, dtype=jnp.float32) * (-2.0 * math.log(rope_base) / head_dim)
    )
    angles = positions.astype(jnp.float32)[:, None] * inv_rates[None, :]
    cosine = jnp.cos(angles)[:, None, :]
    sine_part = jnp.sin(angles)[:, None, :]
    first_half = values[..., :half_dim]
    second = values[..., half_dim:]
    return jnp.concatenate(
        [first_half * cosine - second * sine_part, second * cosine + first_half * sine_part],
        axis=-1,
    )


def pool_rows(offsets, count):
    patch = jnp.arange(CHUNKS * CHUNK, dtype=jnp.int32)
    down, across = patch // 27, patch % 27
    cell = jnp.where(patch < 729, (down // 2) * 14 + across // 2, -1)
    share = jnp.where(down == 26, 1.0, 0.5) * jnp.where(across == 26, 1.0, 0.5)
    is_valid = (offsets >= 0) & (offsets < count)
    hit = is_valid[:, None] & (offsets[:, None] == cell[None, :])
    return jnp.where(hit, share[None, :], 0.0).astype(jnp.bfloat16), is_valid


def per_device(
    patches,
    fc_gain,
    fc_in,
    fc_in_bias,
    fc_out,
    fc_out_bias,
    proj_weight,
    text_embed,
    frame_start,
    frame_count,
    segment_ids,
    norm_gain,
    query_weight,
    query_bias,
    key_weight,
    value_weight,
    value_bias,
):
    shard_id = lax.axis_index("seq")
    shard_rows = text_embed.shape[0]
    head_size = key_weight.shape[1]
    group_size = query_weight.shape[1] // head_size

    def pieces(matrix, width):
        matrix = jnp.pad(matrix, [(0, 32 - matrix.shape[0]), (0, 8 * width - matrix.shape[1])])
        return matrix.reshape(32, 8, width).transpose(1, 0, 2)

    w_in, w_out = fc_in[0], fc_out[0].T
    tail = jnp.stack([w_in[:, 2048:], w_out[:, 2048:]])
    tail = jnp.pad(jnp.tile(tail, (4, 1, 1)), [(0, 0), (0, 14), (0, 0)])
    w = jnp.concatenate([pieces(w_in[:, :2048], 256), pieces(w_out[:, :2048], 256), tail], axis=2)
    p = pieces(proj_weight, 512)
    frame = jnp.pad(patches[0], [(0, CHUNKS * CHUNK - patches.shape[1]), (0, 0)])
    frame = frame.reshape(CHUNKS, CHUNK, patches.shape[2])

    local_slots = jnp.arange(shard_rows, dtype=jnp.int32)
    positions = shard_id * shard_rows + local_slots
    previous = jnp.maximum(shard_id - 1, 0)
    prev_offsets = positions - frame_start[previous]
    prev_valid = (shard_id > 0) & (prev_offsets >= 0) & (prev_offsets < frame_count[previous])
    own_offsets = positions - frame_start[shard_id]
    own_pool, own_valid = pool_rows(own_offsets, frame_count[shard_id])
    next_pool, _ = pool_rows(own_offsets + shard_rows, frame_count[shard_id])
    select = jnp.concatenate([own_pool, next_pool])
    valid = (own_valid | prev_valid).astype(jnp.int32)[:, None]
    inputs = encode(w, p, frame, fc_gain, fc_in_bias, fc_out_bias, select, text_embed, valid)
    widened = inputs.astype(jnp.float32)
    normed = (
        widened
        * lax.rsqrt(jnp.mean(widened * widened, axis=1, keepdims=True) + rms_eps)
        * norm_gain
    ).astype(jnp.bfloat16)
    queries = jnp.dot(normed, query_weight, preferred_element_type=jnp.float32) + query_bias
    queries = rotate(queries.reshape(shard_rows, group_size, head_size), positions).astype(
        jnp.bfloat16
    )
    key_heads = jnp.dot(normed, key_weight, preferred_element_type=jnp.float32)
    key_heads = rotate(key_heads.reshape(shard_rows, 1, head_size), positions).astype(jnp.bfloat16)
    key_heads = key_heads.reshape(shard_rows, head_size)
    values = (
        jnp.dot(normed, value_weight, preferred_element_type=jnp.float32) + value_bias
    ).astype(jnp.bfloat16)
    stacked = jnp.concatenate([key_heads, values], axis=1)
    queries = queries.reshape(shard_rows, group_size, head_size).transpose(1, 0, 2)
    queries = queries.reshape(shard_rows * group_size, head_size)
    half_a, half_b = kv_gather(stacked)
    attended = flash(queries, half_a, half_b, segment_ids, shard_id, shard_rows)
    attended = attended.reshape(group_size, shard_rows, head_size).transpose(1, 0, 2)
    return attended.reshape(shard_rows, group_size * head_size)


def solution(mesh):
    return jax.shard_map(
        per_device,
        mesh=mesh,
        in_specs=(
            P("seq", None, None),
            P("section", None),
            P("section", "seq", None),
            P("section", None),
            P("section", None, "seq"),
            P("section", None),
            P("seq", None),
            P("seq", None),
            P(),
            P(),
            P(),
            P(),
            P(None, "section"),
            P("section"),
            P(None, "section"),
            P(None, "section"),
            P("section"),
        ),
        out_specs=P("seq", "section"),
        check_vma=False,
    )
```

```python
import functools
import math

import jax
import jax.numpy as jnp
from jax import lax
from jax.experimental import pallas as pl
from jax.experimental.pallas import tpu as pltpu
from jax.sharding import PartitionSpec as P

NZ, NX, NC = 8, 4, 2


def seq_id(z, x, c):
    return lax.rem(z + NZ, NZ) * (NX * NC) + lax.rem(x + NX, NX) * NC + c


class Ring:
    def __init__(self, send_sem, recv_sem):
        self.send_sem, self.recv_sem, self.used, self.live = send_sem, recv_sem, 0, []

    def copy(self, sent, got, target, into=None):
        n = self.used
        self.used += 1
        to = {"seq": target} if not isinstance(target, dict) else target
        sems = dict(send_sem=self.send_sem.at[n], recv_sem=self.recv_sem.at[n])
        make = functools.partial(
            pltpu.make_async_remote_copy, device_id=to, device_id_type=pl.DeviceIdType.MESH, **sems)
        out = make(src_ref=sent, dst_ref=sent if into is None else into)
        into = make(src_ref=got, dst_ref=got)
        self.live.append(out)
        return out, into

    def finish(self):
        for out in self.live:
            out.wait_send()


def greet(targets):
    barrier = pltpu.get_barrier_semaphore()
    for t in targets:
        t = {"seq": t} if not isinstance(t, dict) else t
        pl.semaphore_signal(barrier, inc=1, device_id=t, device_id_type=pl.DeviceIdType.MESH)
    pl.semaphore_wait(barrier, len(targets))


def torus_gather(ring, me, a_one, a_many, b_one, b_many, b_like_a=False):
    z, x, c = me
    s = 1 - 2 * c
    zm, zo = seq_id(z + s, x, c), seq_id(z - s, x, c)
    xm, xo = seq_id(z, x + s, c), seq_id(z, x - s, c)
    mate = seq_id(z, x, 1 - c)
    zw = lambda k: lax.rem(z - k * s + 2 * NZ, NZ)
    xw = lambda k: lax.rem(x - k * s + 2 * NX, NX)
    one = {"a": lambda dx, dz: a_one(zw(dz), xw(dx)), "b": lambda dx, dz: b_one(zw(dz), xw(dx))}
    dxs, dzs = (0, 1, -1, 2), (0, 1, -1, 2, -2, 3, -3, 4)
    keys = sorted(
        ((kind, dx, dz) for kind in "ab" for dx in dxs for dz in dzs),
        key=lambda k: (abs(k[1]) + abs(k[2]), k[2 if k[0] == "a" else 1] != 0))
    toward = lambda d: d - 1 if d > 0 else d + 1
    copies, after = {}, {key: [] for key in keys}
    for key in keys:
        kind, dx, dz = key
        along_z = dz != 0 and (kind == "a" or dx == 0)
        if dx == dz == 0:
            continue
        source = (dx, toward(dz)) if along_z else (toward(dx), dz)
        target = (zm if dz > 0 else zo) if along_z else (xm if dx > 0 else xo)
        copies[key] = ring.copy(one[kind](*source), one[kind](dx, dz), target)
        after[(kind, *source)].append(copies[key])
    am = {d: ring.copy(a_many(zw(d), c), a_many(zw(-d), 1 - c), mate) for d in dzs}
    bw, bds, late = (zw, dzs, 2) if b_like_a else (xw, dxs, 4)
    bm = {d: ring.copy(b_many(bw(d), c), b_many(bw(-d), 1 - c), mate) for d in bds}
    stages = []
    for t in range(7):
        stage = []
        for key in keys:
            if abs(key[1]) + abs(key[2]) == t:
                if t:
                    stage.append(copies[key][1].wait_recv)
                stage += [out.start for out, _ in after[key]]
        stage += [am[d][0].start for d in dzs if abs(d) + 2 == t]
        stage += [bm[d][0].start for d in bds if abs(d) + late == t]
        stages.append(stage)
    if b_like_a:
        return stages, {d: (zw(-d), [am[d][1].wait_recv, bm[d][1].wait_recv]) for d in dzs}
    return stages + [[pair[1].wait_recv for pair in (*am.values(), *bm.values())]]


def run(stage):
    for step in stage:
        step()


GATHER_COPIES = 31 + 31 + 8 + 8


def attend_kernel(
    kv_ref, q_ref, qseg_ref, aseg_ref, bseg_ref, o_ref,
    a_ref, b_ref, top_ref, total_ref, acc_ref, send_sem, recv_sem, own_sem,
):
    me_seq = lax.axis_index("seq")
    z, x, c = me_seq // (NX * NC), lax.rem(me_seq // NC, NX), lax.rem(me_seq, NC)
    half = kv_ref.shape[0] // 2
    mine = [
        pltpu.make_async_copy(kv_ref.at[pl.ds(0, half)], a_ref.at[z, x, c], own_sem.at[0]),
        pltpu.make_async_copy(kv_ref.at[pl.ds(half, half)], b_ref.at[z, x, c], own_sem.at[1]),
    ]
    for copy in mine:
        copy.start()
    greet([seq_id(z + 1, x, c), seq_id(z - 1, x, c), seq_id(z, x + 1, c), seq_id(z, x - 1, c), seq_id(z, x, 1 - c)])
    for copy in mine:
        copy.wait()
    ring = Ring(send_sem, recv_sem)
    stages, arrivals = torus_gather(
        ring, (z, x, c),
        lambda zz, xx: a_ref.at[zz, xx, c], lambda zz, cc: a_ref.at[zz, :, cc],
        lambda zz, xx: b_ref.at[zz, xx, c], lambda zz, cc: b_ref.at[zz, :, cc], b_like_a=True)

    rows, head = q_ref.shape
    keys = 8 * half
    q = q_ref[...]
    qseg = qseg_ref[...]
    scale = 1.0 / math.sqrt(head)

    def visit(carried, kv, kseg, extra):
        top, total, acc = carried
        s = lax.dot_general(q, kv[:, :head], (((1,), (1,)), ((), ())), preferred_element_type=jnp.float32)
        allowed = kseg == qseg
        if extra is not None:
            allowed = allowed & extra
        s = jnp.where(allowed, s * scale, -1e30)
        new_top = jnp.maximum(top, jnp.max(s, axis=1, keepdims=True))
        w = jnp.exp(s - new_top)
        if extra is not None:
            w = jnp.where(allowed, w, 0.0)
        keep = jnp.exp(top - new_top)
        total = total * keep + jnp.sum(w, axis=1, keepdims=True)
        acc = acc * keep + jnp.dot(w.astype(jnp.bfloat16), kv[:, head:], preferred_element_type=jnp.float32)
        return new_top, total, acc

    def both(zz, state, first):
        flat = lambda ref: ref[zz].reshape(keys, 2 * head)
        causal = (None, None)
        if first:
            row = lax.broadcasted_iota(jnp.int32, (rows, 1), 0) & 127
            qpos = row + lax.rem(me_seq, NX * NC) * 128
            col = lax.broadcasted_iota(jnp.int32, (1, keys), 1)
            kpos = (col >> 6) * 128 + (col & 63)
            causal = (kpos <= qpos, kpos + half <= qpos)
        state = visit(state, flat(a_ref), aseg_ref[zz], causal[0])
        state = visit(state, flat(b_ref), bseg_ref[zz], causal[1])
        top_ref[...], total_ref[...], acc_ref[...] = state

    def look_at(d):
        source, waits = arrivals[d]
        run(waits)
        if d == 0:
            both(source, (
                jnp.full((rows, 1), -1e30, jnp.float32),
                jnp.zeros((rows, 1), jnp.float32),
                jnp.zeros((rows, head), jnp.float32)), True)
        else:
            @pl.when(source < z)
            def _():
                both(source, (top_ref[...], total_ref[...], acc_ref[...]), False)

    for t, stage in enumerate(stages):
        run(stage)
        for d in (0, 1, -1, 2, -2, 3, -3):
            if abs(d) + 3 == t:
                look_at(d)
    look_at(4)
    o_ref[...] = (acc_ref[...] / total_ref[...]).astype(o_ref.dtype)
    ring.finish()


def attend(q, kv, segment_ids, shard, rows):
    half = rows // 2
    halves = segment_ids.reshape(NZ, NX * NC, 2, half)
    aseg = halves[:, :, 0].reshape(NZ, 1, NX * NC * half)
    bseg = halves[:, :, 1].reshape(NZ, 1, NX * NC * half)
    own = lax.dynamic_slice_in_dim(segment_ids, shard * rows, rows, 0)
    qseg = jnp.tile(own, q.shape[0] // rows)[:, None]
    whole = pl.BlockSpec(memory_space=pltpu.VMEM)
    blocks = pltpu.VMEM((NZ, NX, NC, half, kv.shape[1]), kv.dtype)
    count = q.shape[0]
    return pl.pallas_call(
        attend_kernel,
        out_shape=jax.ShapeDtypeStruct(q.shape, jnp.bfloat16),
        in_specs=[whole] * 5,
        out_specs=whole,
        scratch_shapes=[
            blocks, blocks,
            pltpu.VMEM((count, 1), jnp.float32), pltpu.VMEM((count, 1), jnp.float32), pltpu.VMEM(q.shape, jnp.float32),
            pltpu.SemaphoreType.DMA((GATHER_COPIES,)),
            pltpu.SemaphoreType.DMA((GATHER_COPIES,)),
            pltpu.SemaphoreType.DMA((2,)),
        ],
        compiler_params=pltpu.CompilerParams(collective_id=1, has_side_effects=True, vmem_limit_bytes=48 << 20),
        cost_estimate=pl.CostEstimate(flops=2 * 10**9, bytes_accessed=40_000_000, transcendentals=4_000_000),
        name="attend",
    )(kv, q, qseg, aseg, bseg)


CHUNKS, CHUNK = 8, 96
HEAD_START, EVERY = 2, 2
WIDTH = 256
ENC_COPIES = 7 + 7 + 2 * GATHER_COPIES + 8 + 1 + 6
layer_eps = 1e-06
rms_eps = 1e-06
rope_base = 1000000.0


def encoder_kernel(
    start_ref, count_ref, in_ref, out_ref, proj_ref, patches_ref, gain_ref, bin_ref, bout_ref, text_hbm,
    norm_ref, qw_hbm, kw_hbm, vw_hbm, qb_ref, vb_ref, cos_ref, sin_ref,
    q_ref, kv_ref,
    mixed_ref, qkv_ref,
    w_ref, p_ref, select_ref, frame_ref, text_ref, rec_w, rec_p, win, wout, extra, pa, pb, inflow, outflow, passed, vision,
    send_sem, recv_sem, chunk_send, chunk_recv, cast_send, cast_recv, local_sem,
):
    me_seq, section = lax.axis_index("seq"), lax.axis_index("section")
    z, x, c = me_seq // (NX * NC), lax.rem(me_seq // NC, NX), lax.rem(me_seq, NC)
    j = lax.rem(me_seq, NX * NC)
    last = section == 3
    up, down = lax.rem(section + 1, 4), lax.rem(section + 3, 4)
    shards = NZ * NX * NC
    ahead, behind = lax.rem(me_seq + 1, shards), lax.rem(me_seq + shards - 1, shards)
    others = [lax.rem(j + k, 8) for k in range(8)]
    sources = [lax.rem(j + 8 - k, 8) for k in range(8)]
    member = lambda k: z * (NX * NC) + k

    frame = pltpu.make_async_copy(patches_ref, frame_ref, local_sem.at[2])
    text = pltpu.make_async_copy(text_hbm, text_ref, local_sem.at[11])
    heads = qw_hbm.shape[1]
    head = kw_hbm.shape[1]
    loads = [text] + [
        pltpu.make_async_copy(ref, qkv_ref.at[:, pl.ds(at, ref.shape[1])], local_sem.at[12 + n])
        for n, (ref, at) in enumerate(((qw_hbm, 0), (kw_hbm, heads), (vw_hbm, heads + head)))
    ]
    for copy in loads:
        copy.start()

    @pl.when(section == 0)
    def _():
        frame.start()

    depth = in_ref.shape[0]
    w_ref[:, 16:, :] = jnp.zeros((8, 16, w_ref.shape[2]), w_ref.dtype)
    p_ref[:, 16:, :] = jnp.zeros((8, 16, p_ref.shape[2]), p_ref.dtype)
    p_ref[7] = jnp.zeros(p_ref.shape[1:], p_ref.dtype)
    for k in range(8):
        w_ref[k, :depth, :256] = in_ref[:, 256 * k : 256 * k + 256]
        w_ref[k, :depth, 256:512] = out_ref[:, 256 * k : 256 * k + 256]
        w_ref[k, :depth, 512:] = (out_ref if k % 2 else in_ref)[:, 2048:]
        if k < 7:
            p_ref[k, :depth] = proj_ref[:, 512 * k : 512 * k + 512]
    own = [
        pltpu.make_async_copy(w_ref.at[j], rec_w.at[j], local_sem.at[0]),
        pltpu.make_async_copy(p_ref.at[j], rec_p.at[j], local_sem.at[1]),
    ]
    rows = win.shape[3]
    at = lax.broadcasted_iota(jnp.int32, (rows, 256), 0)
    slot = lax.broadcasted_iota(jnp.int32, (rows, 256), 1)
    inner = slot & 31
    pick = jnp.where((inner < depth) & (at == depth * (slot >> 5) + inner), 1.0, 0.0).astype(jnp.bfloat16)

    greet(
        [member(k) for k in others[1:]]
        + [seq_id(z + 1, x, c), seq_id(z - 1, x, c), ahead, behind, {"section": up}, {"section": down}]
    )
    ring = Ring(send_sem, recv_sem)
    spread_w = [ring.copy(w_ref.at[others[k]], rec_w.at[sources[k]], member(others[k]), rec_w.at[j]) for k in range(1, 8)]
    spread_p = [ring.copy(p_ref.at[others[k]], rec_p.at[sources[k]], member(others[k]), rec_p.at[j]) for k in range(1, 8)]
    for out, _ in spread_w:
        out.start()
    for copy in own:
        copy.start()
    for copy in own:
        copy.wait()
    for _, into in spread_w:
        into.wait_recv()
    block = jnp.dot(pick, rec_w[...].reshape(-1, rec_w.shape[2]), preferred_element_type=jnp.float32)
    block = block.astype(jnp.bfloat16)
    wout[x, c, z] = block[:, 256:512]
    win[x, c, z] = block[:, :256]
    extra[c, z] = block[:, 512:]

    def views(a, b):
        return (
            lambda zz, xx: a.at[xx, c, zz], lambda zz, cc: a.at[:, cc, zz],
            lambda zz, xx: b.at[xx, c, zz], lambda xx, cc: b.at[xx, cc])

    stages = torus_gather(ring, (z, x, c), *views(win, wout))
    s = 1 - 2 * c
    zw = lambda k: lax.rem(z + k + 2 * NZ, NZ)
    zm, zo = seq_id(z + s, x, c), seq_id(z - s, x, c)
    ez_m = [ring.copy(extra.at[c, zw(-k * s)], extra.at[c, zw(-(k + 1) * s)], zm) for k in range(4)]
    ez_o = [ring.copy(extra.at[c, zw(k * s)], extra.at[c, zw((k + 1) * s)], zo) for k in range(3)]
    e_mate = ring.copy(extra.at[c], extra.at[1 - c], seq_id(z, x, 1 - c))
    for n, stage in enumerate(stages):
        if n == 7:
            e_mate[0].start()
        run(stage)
        if n == 2:
            ez_m[0][0].start()
            ez_o[0][0].start()
        if 3 <= n < 7:
            ez_m[n - 3][1].wait_recv()
            if n < 6:
                ez_m[n - 2][0].start()
                ez_o[n - 3][1].wait_recv()
            if n < 5:
                ez_o[n - 2][0].start()
    e_mate[1].wait_recv()
    for out, _ in spread_p:
        out.start()

    def lay_out_p():
        for _, into in spread_p:
            into.wait_recv()
        block = jnp.dot(pick, rec_p[...].reshape(-1, rec_p.shape[2]), preferred_element_type=jnp.float32)
        block = block.astype(jnp.bfloat16)
        pa[x, c, z] = block[:, :256]
        pb[x, c, z] = block[:, 256:]

    p_stages = [[lay_out_p]] + torus_gather(ring, (z, x, c), *views(pa, pb))

    @pl.when(section == 0)
    def _():
        frame.wait()
        full = frame_ref.shape[0] // CHUNK
        for i in range(full):
            inflow[i] = frame_ref[CHUNK * i : CHUNK * i + CHUNK]
        inflow[full] = jnp.zeros((CHUNK, frame_ref.shape[1]), inflow.dtype)
        inflow[full, : frame_ref.shape[0] - CHUNK * full] = frame_ref[CHUNK * full :]

    for n in range(3 * HEAD_START):
        @pl.when(n < HEAD_START * section)
        def _():
            run(p_stages[n])

    count = text_ref.shape[0]
    first, kept = start_ref[me_seq], count_ref[me_seq]

    @pl.when(last)
    def _():
        shape = select_ref.shape
        token = lax.broadcasted_iota(jnp.int32, (shape[0], 1), 0) + (me_seq * count - first)
        patch = lax.broadcasted_iota(jnp.int32, (1, shape[1]), 1)
        down = (patch * 607) >> 14
        across = patch - 27 * down
        cell = jnp.where(patch < 729, (down >> 1) * 14 + (across >> 1), -1)
        share = jnp.where(down == 26, 1.0, 0.5) * jnp.where(across == 26, 1.0, 0.5)
        token = jnp.where((token >= 0) & (token < kept), token, -2)
        select_ref[...] = jnp.where(token == cell, share, 0.0).astype(jnp.bfloat16)

    def chunk_copy(i):
        return pltpu.make_async_remote_copy(
            src_ref=outflow.at[i], dst_ref=inflow.at[i], send_sem=chunk_send.at[i], recv_sem=chunk_recv.at[i],
            device_id={"section": up}, device_id_type=pl.DeviceIdType.MESH)

    def one_chunk(i, nothing):
        @pl.when(section > 0)
        def _():
            chunk_copy(i).wait_recv()

        widened = inflow[i].astype(jnp.float32)
        center = widened - jnp.mean(widened, axis=1, keepdims=True)
        spread = jnp.mean(center * center, axis=1, keepdims=True)
        normed = (center * lax.rsqrt(spread + layer_eps) * gain_ref[...]).astype(jnp.bfloat16)

        def hidden(w_in, b_in):
            v = jnp.dot(normed, w_in, preferred_element_type=jnp.float32) + b_in
            return jax.nn.gelu(v, approximate=True).astype(jnp.bfloat16)

        flat = lambda ref, k: ref[k // 2, k % 2].reshape(8 * rows, 256)
        parts = [hidden(flat(win, k), bin_ref[:, 256 * k : 256 * k + 256]) for k in range(8)]
        parts.append(hidden(extra[0].reshape(8 * rows, 128), bin_ref[:, 2048:]))
        for at in range(0, 8 * rows, WIDTH):
            to = min(at + WIDTH, 8 * rows)
            out = widened[:, at:to] + bout_ref[:, at:to]
            for k in range(9):
                w_out = flat(wout, k) if k < 8 else extra[1].reshape(8 * rows, 128)
                out += lax.dot_general(
                    parts[k], w_out[at:to], (((1,), (1,)), ((), ())), preferred_element_type=jnp.float32)
            outflow[i, :, at:to] = out.astype(jnp.bfloat16)

        @pl.when(jnp.logical_not(last))
        def _():
            chunk_copy(i).start()

        for n, stage in enumerate(p_stages):
            @pl.when((i == EVERY * (n - HEAD_START * section)) & (section > 0))
            def _():
                run(stage)

        return nothing

    lax.fori_loop(0, CHUNKS, one_chunk, 0)

    for n, stage in enumerate(p_stages):
        @pl.when((EVERY * (n - HEAD_START * section) >= CHUNKS) | (section == 0))
        def _():
            run(stage)

    @pl.when(jnp.logical_not(last))
    def _():
        for i in range(CHUNKS):
            chunk_copy(i).wait_send()

    over = pltpu.make_async_remote_copy(
        src_ref=passed.at[0], dst_ref=passed.at[1], send_sem=local_sem.at[3], recv_sem=local_sem.at[4],
        device_id={"seq": ahead}, device_id_type=pl.DeviceIdType.MESH)
    parts = vision.shape[0]
    cast = lambda h, n, to: pltpu.make_async_remote_copy(
        src_ref=vision.at[h], dst_ref=vision.at[h], send_sem=cast_send.at[n], recv_sem=cast_recv.at[h],
        device_id={"section": to}, device_id_type=pl.DeviceIdType.MESH)

    @pl.when(last)
    def _():
        encoded = outflow[...].reshape(CHUNKS * CHUNK, outflow.shape[2])
        passed[0] = jnp.dot(select_ref[count:], encoded, preferred_element_type=jnp.float32).astype(jnp.bfloat16)
        over.start()
        mine = jnp.dot(select_ref[:count], encoded, preferred_element_type=jnp.float32)
        over.wait()
        mine = mine + jnp.where(me_seq > 0, passed[1].astype(jnp.float32), 0.0)
        vision[...] = mine.astype(jnp.bfloat16).reshape(vision.shape)
        copies = []
        for h in range(parts):
            copies += [cast(h, h, 0), cast(parts - 1 - h, parts + h, 2)]
        for copy in copies:
            copy.start()
        for copy in copies:
            copy.wait_send()

    for me, order in ((0, range(parts)), (2, range(parts - 1, -1, -1))):
        @pl.when(section == me)
        def _():
            for h in list(order)[: parts // 2]:
                cast(h, h, 1).wait_recv()
                cast(h, h, 1).start()
            for h in list(order)[parts // 2 :]:
                cast(h, h, 1).wait_recv()
            for h in list(order)[: parts // 2]:
                cast(h, h, 1).wait_send()

    @pl.when(section == 1)
    def _():
        for h in range(parts):
            cast(h, h, 1).wait_recv()

    tokens = vision[...].reshape(count, vision.shape[2])
    for copy in loads:
        copy.wait()
    slots = lax.broadcasted_iota(jnp.int32, (count, 1), 0) + me_seq * count
    before = jnp.maximum(me_seq - 1, 0)
    prior = slots - start_ref[before]
    valid = (slots >= first) & (slots < first + kept)
    valid = valid | ((me_seq > 0) & (prior >= 0) & (prior < count_ref[before]))
    squares = jnp.zeros((count, 1), jnp.float32)
    for k in range(7):
        for n, ref in enumerate((pa, pb)):
            out = jnp.dot(tokens, ref[k // 2, k % 2].reshape(8 * rows, 256), preferred_element_type=jnp.float32)
            at = 512 * k + 256 * n
            out = jnp.where(valid, out.astype(jnp.bfloat16), text_ref[:, at : at + 256])
            mixed_ref[:, at : at + 256] = out
            out = out.astype(jnp.float32)
            squares += jnp.sum(out * out, axis=1, keepdims=True)
    factor = lax.rsqrt(squares / mixed_ref.shape[1] + rms_eps)
    normed = (mixed_ref[...].astype(jnp.float32) * factor * norm_ref[...]).astype(jnp.bfloat16)
    rope = lambda u: u * cos_ref[...] + pltpu.roll(u, head // 2, 1) * sin_ref[...]
    for n in range(0, heads, 2 * head):
        two = jnp.dot(normed, qkv_ref[:, n : n + 2 * head], preferred_element_type=jnp.float32)
        two = two + qb_ref[:, n : n + 2 * head]
        for i in range(2):
            at = (n // head + i) * count
            q_ref[at : at + count] = rope(two[:, i * head : (i + 1) * head]).astype(jnp.bfloat16)
    two = jnp.dot(normed, qkv_ref[:, heads:], preferred_element_type=jnp.float32)
    kv_ref[:, :head] = rope(two[:, :head]).astype(jnp.bfloat16)
    kv_ref[:, head:] = (two[:, head:] + vb_ref[...]).astype(jnp.bfloat16)
    ring.finish()


def encode(start, kept, w_in, w_out, proj, patches, gain, b_in, b_out, text, norm, qw, kw, vw, qb, vb, cos, sin):
    rows, width = 8 * w_in.shape[0], patches.shape[1]
    whole = pl.BlockSpec(memory_space=pltpu.VMEM)
    scalars = pl.BlockSpec(memory_space=pltpu.SMEM)
    away = pl.BlockSpec(memory_space=pl.ANY)
    bf = jnp.bfloat16
    big = pltpu.VMEM((NX, NC, NZ, rows, 256), bf)
    spread = [pltpu.VMEM((8, 32, 640), bf), pltpu.VMEM((8, 32, 512), bf)]
    return pl.pallas_call(
        encoder_kernel,
        out_shape=(
            jax.ShapeDtypeStruct((text.shape[0] * (qw.shape[1] // kw.shape[1]), kw.shape[1]), bf),
            jax.ShapeDtypeStruct((text.shape[0], 2 * kw.shape[1]), bf),
        ),
        in_specs=[scalars, scalars, whole, whole, whole, away, whole, whole, whole, away]
        + [whole, away, away, away] + [whole] * 4,
        out_specs=(whole, whole),
        scratch_shapes=[
            pltpu.VMEM(text.shape, bf), pltpu.VMEM((text.shape[1], qw.shape[1] + 2 * kw.shape[1]), bf),
            *spread, pltpu.VMEM((2 * text.shape[0], CHUNKS * CHUNK), bf),
            pltpu.VMEM(patches.shape, bf), pltpu.VMEM(text.shape, bf), *spread,
            big, big, pltpu.VMEM((NC, NZ, rows, 128), bf), big, big,
            pltpu.VMEM((CHUNKS, CHUNK, width), bf), pltpu.VMEM((CHUNKS, CHUNK, width), bf),
            pltpu.VMEM((2, text.shape[0], width), bf), pltpu.VMEM((4, text.shape[0] // 4, width), bf),
            pltpu.SemaphoreType.DMA((ENC_COPIES,)), pltpu.SemaphoreType.DMA((ENC_COPIES,)),
            pltpu.SemaphoreType.DMA((CHUNKS,)), pltpu.SemaphoreType.DMA((CHUNKS,)),
            pltpu.SemaphoreType.DMA((8,)), pltpu.SemaphoreType.DMA((4,)),
            pltpu.SemaphoreType.DMA((16,)),
        ],
        compiler_params=pltpu.CompilerParams(collective_id=0, has_side_effects=True, vmem_limit_bytes=60 << 20),
        cost_estimate=pl.CostEstimate(flops=10**10, bytes_accessed=40_000_000, transcendentals=2_000_000),
        name="encode",
    )(start, kept, w_in, w_out, proj, patches, gain, b_in, b_out, text, norm, qw, kw, vw, qb, vb, cos, sin)


def per_device(
    patches,
    fc_gain,
    fc_in,
    fc_in_bias,
    fc_out,
    fc_out_bias,
    proj_weight,
    text_embed,
    frame_start,
    frame_count,
    segment_ids,
    norm_gain,
    query_weight,
    query_bias,
    key_weight,
    value_weight,
    value_bias,
):
    shard_id = lax.axis_index("seq")
    shard_rows = text_embed.shape[0]
    head_size = key_weight.shape[1]
    group_size = query_weight.shape[1] // head_size

    local_slots = jnp.arange(shard_rows, dtype=jnp.int32)
    positions = shard_id * shard_rows + local_slots
    half_dim = head_size // 2
    inv_rates = jnp.exp(
        jnp.arange(half_dim, dtype=jnp.float32) * (-2.0 * math.log(rope_base) / head_size)
    )
    angles = positions.astype(jnp.float32)[:, None] * inv_rates[None, :]
    cosine, sine = jnp.cos(angles), jnp.sin(angles)
    queries, stacked = encode(
        frame_start, frame_count, fc_in[0], fc_out[0].T, proj_weight, patches[0],
        fc_gain, fc_in_bias, fc_out_bias, text_embed,
        norm_gain[None], query_weight, key_weight, value_weight, query_bias[None], value_bias[None],
        jnp.concatenate([cosine, cosine], axis=1), jnp.concatenate([-sine, sine], axis=1),
    )
    attended = attend(queries, stacked, segment_ids, shard_id, shard_rows)
    attended = attended.reshape(group_size, shard_rows, head_size).transpose(1, 0, 2)
    return attended.reshape(shard_rows, group_size * head_size)


def solution(mesh):
    return jax.shard_map(
        per_device,
        mesh=mesh,
        in_specs=(
            P("seq", None, None),
            P("section", None),
            P("section", "seq", None),
            P("section", None),
            P("section", None, "seq"),
            P("section", None),
            P("seq", None),
            P("seq", None),
            P(),
            P(),
            P(),
            P(),
            P(None, "section"),
            P("section"),
            P(None, "section"),
            P(None, "section"),
            P("section"),
        ),
        out_specs=P("seq", "section"),
        check_vma=False,
    )
```

```python
import functools
import math

import jax
import jax.numpy as jnp
from jax import lax
from jax.experimental import pallas as pl
from jax.experimental.pallas import tpu as pltpu
from jax.sharding import PartitionSpec as P

NZ, NX, NC = 8, 4, 2


def seq_id(z, x, c):
    return lax.rem(z + NZ, NZ) * (NX * NC) + lax.rem(x + NX, NX) * NC + c


class Ring:
    def __init__(self, send_sem, recv_sem):
        self.send_sem, self.recv_sem, self.used, self.live = send_sem, recv_sem, 0, []

    def copy(self, sent, got, target, into=None):
        n = self.used
        self.used += 1
        to = {"seq": target} if not isinstance(target, dict) else target
        sems = dict(send_sem=self.send_sem.at[n], recv_sem=self.recv_sem.at[n])
        make = functools.partial(
            pltpu.make_async_remote_copy, device_id=to, device_id_type=pl.DeviceIdType.MESH, **sems)
        out = make(src_ref=sent, dst_ref=sent if into is None else into)
        into = make(src_ref=got, dst_ref=got)
        self.live.append(out)
        return out, into

    def finish(self):
        for out in self.live:
            out.wait_send()


def greet(targets):
    barrier = pltpu.get_barrier_semaphore()
    for t in targets:
        t = {"seq": t} if not isinstance(t, dict) else t
        pl.semaphore_signal(barrier, inc=1, device_id=t, device_id_type=pl.DeviceIdType.MESH)
    pl.semaphore_wait(barrier, len(targets))


def torus_gather(ring, me, a_one, a_many, b_one, b_many, b_like_a=False):
    z, x, c = me
    s = 1 - 2 * c
    zm, zo = seq_id(z + s, x, c), seq_id(z - s, x, c)
    xm, xo = seq_id(z, x + s, c), seq_id(z, x - s, c)
    mate = seq_id(z, x, 1 - c)
    zw = lambda k: lax.rem(z - k * s + 2 * NZ, NZ)
    xw = lambda k: lax.rem(x - k * s + 2 * NX, NX)
    one = {"a": lambda dx, dz: a_one(zw(dz), xw(dx)), "b": lambda dx, dz: b_one(zw(dz), xw(dx))}
    dxs, dzs = (0, 1, -1, 2), (0, 1, -1, 2, -2, 3, -3, 4)
    keys = sorted(
        ((kind, dx, dz) for kind in "ab" for dx in dxs for dz in dzs),
        key=lambda k: (abs(k[1]) + abs(k[2]), k[2 if k[0] == "a" else 1] != 0))
    toward = lambda d: d - 1 if d > 0 else d + 1
    copies, after = {}, {key: [] for key in keys}
    for key in keys:
        kind, dx, dz = key
        along_z = dz != 0 and (kind == "a" or dx == 0)
        if dx == dz == 0:
            continue
        source = (dx, toward(dz)) if along_z else (toward(dx), dz)
        target = (zm if dz > 0 else zo) if along_z else (xm if dx > 0 else xo)
        copies[key] = [ring.copy(sent, got, target) for sent, got in zip(one[kind](*source), one[kind](dx, dz))]
        after[(kind, *source)] += copies[key]
    am = {d: ring.copy(a_many(zw(d), c), a_many(zw(-d), 1 - c), mate) for d in dzs}
    bw, bds, late = (zw, dzs, 2) if b_like_a else (xw, dxs, 4)
    bm = {d: ring.copy(b_many(bw(d), c), b_many(bw(-d), 1 - c), mate) for d in bds}
    stages = []
    for t in range(7):
        stage = []
        for key in keys:
            if abs(key[1]) + abs(key[2]) == t:
                if t:
                    stage += [into.wait_recv for _, into in copies[key]]
                stage += [out.start for out, _ in after[key]]
        stage += [am[d][0].start for d in dzs if abs(d) + 2 == t]
        stage += [bm[d][0].start for d in bds if abs(d) + late == t]
        stages.append(stage)
    if b_like_a:
        return stages, {d: (zw(-d), [am[d][1].wait_recv, bm[d][1].wait_recv]) for d in dzs}
    return stages + [[pair[1].wait_recv for pair in (*am.values(), *bm.values())]]


def run(stage):
    for step in stage:
        step()


GATHER_COPIES = 31 + 31 + 8 + 8


def attend_kernel(
    kv_ref, q_hbm, qseg_ref, kseg_ref, o_ref,
    q_ref, a_ref, b_ref, top_ref, total_ref, acc_ref, send_sem, recv_sem, own_sem,
):
    me_seq = lax.axis_index("seq")
    z, x, c = me_seq // (NX * NC), lax.rem(me_seq // NC, NX), lax.rem(me_seq, NC)
    half = kv_ref.shape[0] // 2
    mine = [
        pltpu.make_async_copy(kv_ref.at[pl.ds(0, half)], a_ref.at[z, x, c], own_sem.at[0]),
        pltpu.make_async_copy(kv_ref.at[pl.ds(half, half)], b_ref.at[z, x, c], own_sem.at[1]),
    ]
    for copy in mine:
        copy.start()
    queries = pltpu.make_async_copy(q_hbm, q_ref, own_sem.at[2])
    queries.start()
    greet([seq_id(z + 1, x, c), seq_id(z - 1, x, c), seq_id(z, x + 1, c), seq_id(z, x - 1, c), seq_id(z, x, 1 - c)])
    for copy in mine:
        copy.wait()
    ring = Ring(send_sem, recv_sem)
    stages, arrivals = torus_gather(
        ring, (z, x, c),
        lambda zz, xx: (a_ref.at[zz, xx, c],), lambda zz, cc: a_ref.at[zz, :, cc],
        lambda zz, xx: (b_ref.at[zz, xx, c],), lambda zz, cc: b_ref.at[zz, :, cc], b_like_a=True)

    rows, head = q_ref.shape
    queries.wait()
    q = q_ref[...]
    qseg = qseg_ref[...]
    scale = math.log2(math.e) / math.sqrt(head)

    def visit(zz, cc, first):
        kv = [ref[zz, :, cc].reshape(NX * half, 2 * head) for ref in (a_ref, b_ref)]
        allowed = [kseg_ref[zz, cc, n : n + 1] == qseg for n in range(2)]
        if first:
            row = lax.broadcasted_iota(jnp.int32, (rows, 1), 0) & 127
            qpos = row + lax.rem(me_seq, NX * NC) * 128
            col = lax.broadcasted_iota(jnp.int32, (1, NX * half), 1)
            kpos = (col >> 6) * 256 + cc * 128 + (col & 63)
            allowed = [ok & (kpos + n * half <= qpos) for n, ok in enumerate(allowed)]
        scores = [
            lax.dot_general(q, one[:, :head], (((1,), (1,)), ((), ())), preferred_element_type=jnp.float32)
            for one in kv
        ]
        scores = [jnp.where(ok, s * scale, -1e30) for s, ok in zip(scores, allowed)]
        top = jnp.max(jnp.maximum(*scores), axis=1, keepdims=True)
        if not (first and cc is c):
            top = jnp.maximum(top_ref[...], top)
        weights = [jnp.exp2(s - top) for s in scores]
        total = jnp.sum(weights[0] + weights[1], axis=1, keepdims=True)
        acc = sum(
            jnp.dot(w.astype(jnp.bfloat16), one[:, head:], preferred_element_type=jnp.float32)
            for w, one in zip(weights, kv))
        if not (first and cc is c):
            keep = jnp.exp2(top_ref[...] - top)
            total += total_ref[...] * keep
            acc += acc_ref[...] * keep
        top_ref[...], total_ref[...], acc_ref[...] = top, total, acc

    def look_at(d, cc):
        source, waits = arrivals[d]
        if cc is not c:
            run(waits)
        if d == 0:
            visit(source, cc, True)
        else:
            @pl.when(source < z)
            def _():
                visit(source, cc, False)

    other = 1 - c
    ds = (0, 1, -1, 2, -2, 3, -3, 4)
    for t, stage in enumerate(stages):
        run(stage)
        for d in ds:
            if abs(d) + 3 == t:
                look_at(d, other)
        for d in ds:
            if abs(d) + 2 == t:
                look_at(-d if d != 4 else 4, c)
    look_at(4, other)
    o_ref[...] = (acc_ref[...] / total_ref[...]).astype(o_ref.dtype)
    ring.finish()


def attend(q, kv, segment_ids, shard, rows):
    half = rows // 2
    kseg = segment_ids.reshape(NZ, NX, NC, 2, half).transpose(0, 2, 3, 1, 4).reshape(NZ, NC, 2, NX * half)
    own = lax.dynamic_slice_in_dim(segment_ids, shard * rows, rows, 0)
    qseg = jnp.tile(own, q.shape[0] // rows)[:, None]
    whole = pl.BlockSpec(memory_space=pltpu.VMEM)
    blocks = pltpu.VMEM((NZ, NX, NC, half, kv.shape[1]), kv.dtype)
    count = q.shape[0]
    return pl.pallas_call(
        attend_kernel,
        out_shape=jax.ShapeDtypeStruct(q.shape, jnp.bfloat16),
        in_specs=[pl.BlockSpec(memory_space=pl.ANY)] * 2 + [whole] * 2,
        out_specs=whole,
        scratch_shapes=[
            pltpu.VMEM(q.shape, q.dtype), blocks, blocks,
            pltpu.VMEM((count, 1), jnp.float32), pltpu.VMEM((count, 1), jnp.float32), pltpu.VMEM(q.shape, jnp.float32),
            pltpu.SemaphoreType.DMA((GATHER_COPIES,)),
            pltpu.SemaphoreType.DMA((GATHER_COPIES,)),
            pltpu.SemaphoreType.DMA((3,)),
        ],
        compiler_params=pltpu.CompilerParams(collective_id=1, has_side_effects=True, vmem_limit_bytes=48 << 20),
        cost_estimate=pl.CostEstimate(flops=2 * 10**9, bytes_accessed=40_000_000, transcendentals=4_000_000),
        name="attend",
    )(kv, q, qseg, kseg)


CHUNKS, CHUNK = 8, 96
HEAD_START, EVERY = 2, 2
WIDTH = 1152
SPLIT = 112
ENC_COPIES = 14 + 2 * (3 * 31 + 12) + 8
layer_eps = 1e-06
rms_eps = 1e-06
rope_base = 1000000.0


def encoder_kernel(
    start_ref, count_ref, in_ref, out_ref, proj_ref, patches_ref, gain_ref, bin_ref, bout_ref, text_hbm,
    norm_ref, qw_hbm, kw_hbm, vw_hbm, qb_ref, vb_ref, cos_ref, sin_ref,
    q_ref, kv_ref,
    mixed_ref, qkv_ref,
    w_ref, p_ref, select_ref, frame_ref, text_ref, rec_w, rec_p, win, wout, extra, pa, pb, inflow, outflow, passed, vision,
    send_sem, recv_sem, chunk_send, chunk_recv, cast_send, cast_recv, over_send, over_recv, local_sem,
):
    me_seq, section = lax.axis_index("seq"), lax.axis_index("section")
    z, x, c = me_seq // (NX * NC), lax.rem(me_seq // NC, NX), lax.rem(me_seq, NC)
    j = lax.rem(me_seq, NX * NC)
    last = section == 3
    up, down = lax.rem(section + 1, 4), lax.rem(section + 3, 4)
    shards = NZ * NX * NC
    ahead, behind = lax.rem(me_seq + 1, shards), lax.rem(me_seq + shards - 1, shards)
    others = [lax.rem(j + k, 8) for k in range(8)]
    sources = [lax.rem(j + 8 - k, 8) for k in range(8)]
    member = lambda k: z * (NX * NC) + k

    frame = pltpu.make_async_copy(patches_ref, frame_ref, local_sem.at[2])
    text = pltpu.make_async_copy(text_hbm, text_ref, local_sem.at[11])
    heads = qw_hbm.shape[1]
    head = kw_hbm.shape[1]
    loads = [text] + [
        pltpu.make_async_copy(ref, qkv_ref.at[:, pl.ds(at, ref.shape[1])], local_sem.at[12 + n])
        for n, (ref, at) in enumerate(((qw_hbm, 0), (kw_hbm, heads), (vw_hbm, heads + head)))
    ]
    for copy in loads:
        copy.start()

    @pl.when(section == 0)
    def _():
        frame.start()

    depth = in_ref.shape[0]
    w_ref[:, 16:, :] = jnp.zeros((8, 16, w_ref.shape[2]), w_ref.dtype)
    p_ref[:, 16:, :] = jnp.zeros((8, 16, p_ref.shape[2]), p_ref.dtype)
    p_ref[7] = jnp.zeros(p_ref.shape[1:], p_ref.dtype)
    for k in range(8):
        w_ref[k, :depth, :256] = in_ref[:, 256 * k : 256 * k + 256]
        w_ref[k, :depth, 256:512] = out_ref[:, 256 * k : 256 * k + 256]
        w_ref[k, :depth, 512:] = (out_ref if k % 2 else in_ref)[:, 2048:]
        if k < 7:
            p_ref[k, :depth] = proj_ref[:, 512 * k : 512 * k + 512]
    own = [
        pltpu.make_async_copy(w_ref.at[j], rec_w.at[j], local_sem.at[0]),
        pltpu.make_async_copy(p_ref.at[j], rec_p.at[j], local_sem.at[1]),
    ]
    rows = win.shape[3]
    at = lax.broadcasted_iota(jnp.int32, (rows, 256), 0)
    slot = lax.broadcasted_iota(jnp.int32, (rows, 256), 1)
    inner = slot & 31
    pick = jnp.where((inner < depth) & (at == depth * (slot >> 5) + inner), 1.0, 0.0).astype(jnp.bfloat16)

    greet(
        [member(k) for k in others[1:]]
        + [seq_id(z + 1, x, c), seq_id(z - 1, x, c), ahead, behind, {"section": up}, {"section": down}]
    )
    ring = Ring(send_sem, recv_sem)
    spread_w = [ring.copy(w_ref.at[others[k]], rec_w.at[sources[k]], member(others[k]), rec_w.at[j]) for k in range(1, 8)]
    spread_p = [ring.copy(p_ref.at[others[k]], rec_p.at[sources[k]], member(others[k]), rec_p.at[j]) for k in range(1, 8)]
    for out, _ in spread_w:
        out.start()
    for copy in own:
        copy.start()
    for copy in own:
        copy.wait()
    for _, into in spread_w:
        into.wait_recv()
    block = jnp.dot(pick, rec_w[...].reshape(-1, rec_w.shape[2]), preferred_element_type=jnp.float32)
    block = block.astype(jnp.bfloat16)
    wout[x, c, z] = block[:, 256:512]
    win[x, c, z] = block[:, :256]
    extra[c, z] = block[:, 512:]

    def views(a, b):
        return (
            lambda zz, xx: (a.at[xx, c, zz, pl.ds(0, SPLIT)],),
            lambda zz, cc: a.at[:, cc, zz],
            lambda zz, xx: (b.at[xx, c, zz], a.at[xx, c, zz, pl.ds(SPLIT, rows - SPLIT)]),
            lambda xx, cc: b.at[xx, cc])

    stages = torus_gather(ring, (z, x, c), *views(win, wout))
    s = 1 - 2 * c
    zw = lambda k: lax.rem(z + k + 2 * NZ, NZ)
    zm, zo = seq_id(z + s, x, c), seq_id(z - s, x, c)
    ez_m = [ring.copy(extra.at[c, zw(-k * s)], extra.at[c, zw(-(k + 1) * s)], zm) for k in range(4)]
    ez_o = [ring.copy(extra.at[c, zw(k * s)], extra.at[c, zw((k + 1) * s)], zo) for k in range(3)]
    e_mate = ring.copy(extra.at[c], extra.at[1 - c], seq_id(z, x, 1 - c))
    for n, stage in enumerate(stages):
        if n == 7:
            e_mate[0].start()
        run(stage)
        if n == 2:
            ez_m[0][0].start()
            ez_o[0][0].start()
        if 3 <= n < 7:
            ez_m[n - 3][1].wait_recv()
            if n < 6:
                ez_m[n - 2][0].start()
                ez_o[n - 3][1].wait_recv()
            if n < 5:
                ez_o[n - 2][0].start()
    e_mate[1].wait_recv()
    for out, _ in spread_p:
        out.start()

    def lay_out_p():
        for _, into in spread_p:
            into.wait_recv()
        block = jnp.dot(pick, rec_p[...].reshape(-1, rec_p.shape[2]), preferred_element_type=jnp.float32)
        block = block.astype(jnp.bfloat16)
        pa[x, c, z] = block[:, :256]
        pb[x, c, z] = block[:, 256:]

    p_stages = [[lay_out_p]] + torus_gather(ring, (z, x, c), *views(pa, pb))

    @pl.when(section == 0)
    def _():
        frame.wait()
        full = frame_ref.shape[0] // CHUNK
        for i in range(full):
            inflow[i] = frame_ref[CHUNK * i : CHUNK * i + CHUNK]
        inflow[full] = jnp.zeros((CHUNK, frame_ref.shape[1]), inflow.dtype)
        inflow[full, : frame_ref.shape[0] - CHUNK * full] = frame_ref[CHUNK * full :]

    for n in range(3 * HEAD_START):
        @pl.when(n < HEAD_START * section)
        def _():
            run(p_stages[n])

    count = text_ref.shape[0]
    first, kept = start_ref[me_seq], count_ref[me_seq]

    @pl.when(last)
    def _():
        shape = select_ref.shape
        token = lax.broadcasted_iota(jnp.int32, (shape[0], 1), 0) + (me_seq * count - first)
        patch = lax.broadcasted_iota(jnp.int32, (1, shape[1]), 1)
        down = (patch * 607) >> 14
        across = patch - 27 * down
        cell = jnp.where(patch < 729, (down >> 1) * 14 + (across >> 1), -1)
        share = jnp.where(down == 26, 1.0, 0.5) * jnp.where(across == 26, 1.0, 0.5)
        token = jnp.where((token >= 0) & (token < kept), token, -2)
        select_ref[...] = jnp.where(token == cell, share, 0.0).astype(jnp.bfloat16)

    columns = [(at, min(WIDTH, 8 * rows - at)) for at in range(0, 8 * rows, WIDTH)]

    def chunk_copy(i, n):
        at, size = columns[n]
        return pltpu.make_async_remote_copy(
            src_ref=outflow.at[i, :, pl.ds(at, size)], dst_ref=inflow.at[i, :, pl.ds(at, size)],
            send_sem=chunk_send.at[i, n], recv_sem=chunk_recv.at[i, n],
            device_id={"section": up}, device_id_type=pl.DeviceIdType.MESH)

    def one_chunk(i, nothing):
        @pl.when(section > 0)
        def _():
            for n in range(len(columns)):
                chunk_copy(i, n).wait_recv()

        widened = inflow[i].astype(jnp.float32)
        center = widened - jnp.mean(widened, axis=1, keepdims=True)
        spread = jnp.mean(center * center, axis=1, keepdims=True)
        normed = (center * lax.rsqrt(spread + layer_eps) * gain_ref[...]).astype(jnp.bfloat16)

        def hidden(w_in, b_in):
            v = jnp.dot(normed, w_in, preferred_element_type=jnp.float32) + b_in
            return jax.nn.gelu(v, approximate=True).astype(jnp.bfloat16)

        flat = lambda ref, k: ref[k // 2, k % 2].reshape(8 * rows, 256)
        parts = [hidden(flat(win, k), bin_ref[:, 256 * k : 256 * k + 256]) for k in range(8)]
        parts.append(hidden(extra[0].reshape(8 * rows, 128), bin_ref[:, 2048:]))
        for n, (at, size) in enumerate(columns):
            to = at + size
            out = widened[:, at:to] + bout_ref[:, at:to]
            for k in range(9):
                w_out = flat(wout, k) if k < 8 else extra[1].reshape(8 * rows, 128)
                out += lax.dot_general(
                    parts[k], w_out[at:to], (((1,), (1,)), ((), ())), preferred_element_type=jnp.float32)
            outflow[i, :, at:to] = out.astype(jnp.bfloat16)

            @pl.when(jnp.logical_not(last))
            def _():
                chunk_copy(i, n).start()

        for n, stage in enumerate(p_stages):
            @pl.when((i == EVERY * (n - HEAD_START * section)) & (section > 0))
            def _():
                run(stage)

        return nothing

    lax.fori_loop(0, CHUNKS, one_chunk, 0)

    for n, stage in enumerate(p_stages):
        @pl.when((EVERY * (n - HEAD_START * section) >= CHUNKS) | (section == 0))
        def _():
            run(stage)

    @pl.when(jnp.logical_not(last))
    def _():
        for i in range(CHUNKS):
            for n in range(len(columns)):
                chunk_copy(i, n).wait_send()

    over = lambda h: pltpu.make_async_remote_copy(
        src_ref=passed.at[0, h], dst_ref=passed.at[1, h], send_sem=over_send.at[h], recv_sem=over_recv.at[h],
        device_id={"seq": ahead}, device_id_type=pl.DeviceIdType.MESH)
    parts = vision.shape[0]
    order, handed = (0, 3, 1, 2), {0: (0, 1), 2: (3, 2)}
    cast = lambda h, n, to: pltpu.make_async_remote_copy(
        src_ref=vision.at[h], dst_ref=vision.at[h], send_sem=cast_send.at[n], recv_sem=cast_recv.at[h],
        device_id={"section": to}, device_id_type=pl.DeviceIdType.MESH)

    @pl.when(last)
    def _():
        encoded = outflow[...].reshape(CHUNKS * CHUNK, outflow.shape[2])
        out = jnp.dot(select_ref[count:], encoded, preferred_element_type=jnp.float32)
        passed[0] = out.astype(jnp.bfloat16).reshape(vision.shape)
        for h in order:
            over(h).start()
        mine = jnp.dot(select_ref[:count], encoded, preferred_element_type=jnp.float32)
        mine = mine.reshape(vision.shape)
        for h in order:
            over(h).wait_recv()
            other = jnp.where(me_seq > 0, passed[1, h].astype(jnp.float32), 0.0)
            vision[h] = (mine[h] + other).astype(jnp.bfloat16)
            cast(h, h, 0).start()
            cast(h, parts + h, 2).start()
        for h in order:
            over(h).wait_send()
            cast(h, h, 0).wait_send()
            cast(h, parts + h, 2).wait_send()

    for me, mine in handed.items():
        @pl.when(section == me)
        def _():
            for h in order:
                cast(h, h, 1).wait_recv()
                if h in mine:
                    cast(h, h, 1).start()
            for h in mine:
                cast(h, h, 1).wait_send()

    @pl.when(section == 1)
    def _():
        for h in range(parts):
            cast(h, h, 1).wait_recv()

    tokens = vision[...].reshape(count, vision.shape[2])
    for copy in loads:
        copy.wait()
    slots = lax.broadcasted_iota(jnp.int32, (count, 1), 0) + me_seq * count
    before = jnp.maximum(me_seq - 1, 0)
    prior = slots - start_ref[before]
    valid = (slots >= first) & (slots < first + kept)
    valid = valid | ((me_seq > 0) & (prior >= 0) & (prior < count_ref[before]))
    squares = jnp.zeros((count, 1), jnp.float32)
    for k in range(7):
        for n, ref in enumerate((pa, pb)):
            out = jnp.dot(tokens, ref[k // 2, k % 2].reshape(8 * rows, 256), preferred_element_type=jnp.float32)
            at = 512 * k + 256 * n
            out = jnp.where(valid, out.astype(jnp.bfloat16), text_ref[:, at : at + 256])
            mixed_ref[:, at : at + 256] = out
            out = out.astype(jnp.float32)
            squares += jnp.sum(out * out, axis=1, keepdims=True)
    factor = lax.rsqrt(squares / mixed_ref.shape[1] + rms_eps)
    normed = (mixed_ref[...].astype(jnp.float32) * factor * norm_ref[...]).astype(jnp.bfloat16)
    rope = lambda u: u * cos_ref[...] + pltpu.roll(u, head // 2, 1) * sin_ref[...]
    for n in range(0, heads, 2 * head):
        two = jnp.dot(normed, qkv_ref[:, n : n + 2 * head], preferred_element_type=jnp.float32)
        two = two + qb_ref[:, n : n + 2 * head]
        for i in range(2):
            at = (n // head + i) * count
            q_ref[at : at + count] = rope(two[:, i * head : (i + 1) * head]).astype(jnp.bfloat16)
    two = jnp.dot(normed, qkv_ref[:, heads:], preferred_element_type=jnp.float32)
    kv_ref[:, :head] = rope(two[:, :head]).astype(jnp.bfloat16)
    kv_ref[:, head:] = (two[:, head:] + vb_ref[...]).astype(jnp.bfloat16)
    ring.finish()


def encode(start, kept, w_in, w_out, proj, patches, gain, b_in, b_out, text, norm, qw, kw, vw, qb, vb, cos, sin):
    rows, width = 8 * w_in.shape[0], patches.shape[1]
    whole = pl.BlockSpec(memory_space=pltpu.VMEM)
    scalars = pl.BlockSpec(memory_space=pltpu.SMEM)
    away = pl.BlockSpec(memory_space=pl.ANY)
    bf = jnp.bfloat16
    big = pltpu.VMEM((NX, NC, NZ, rows, 256), bf)
    spread = [pltpu.VMEM((8, 32, 640), bf), pltpu.VMEM((8, 32, 512), bf)]
    return pl.pallas_call(
        encoder_kernel,
        out_shape=(
            jax.ShapeDtypeStruct((text.shape[0] * (qw.shape[1] // kw.shape[1]), kw.shape[1]), bf),
            jax.ShapeDtypeStruct((text.shape[0], 2 * kw.shape[1]), bf),
        ),
        in_specs=[scalars, scalars, whole, whole, whole, away, whole, whole, whole, away]
        + [whole, away, away, away] + [whole] * 4,
        out_specs=(whole, whole),
        scratch_shapes=[
            pltpu.VMEM(text.shape, bf), pltpu.VMEM((text.shape[1], qw.shape[1] + 2 * kw.shape[1]), bf),
            *spread, pltpu.VMEM((2 * text.shape[0], CHUNKS * CHUNK), bf),
            pltpu.VMEM(patches.shape, bf), pltpu.VMEM(text.shape, bf), *spread,
            big, big, pltpu.VMEM((NC, NZ, rows, 128), bf), big, big,
            pltpu.VMEM((CHUNKS, CHUNK, width), bf), pltpu.VMEM((CHUNKS, CHUNK, width), bf),
            pltpu.VMEM((2, 4, text.shape[0] // 4, width), bf), pltpu.VMEM((4, text.shape[0] // 4, width), bf),
            pltpu.SemaphoreType.DMA((ENC_COPIES,)), pltpu.SemaphoreType.DMA((ENC_COPIES,)),
            pltpu.SemaphoreType.DMA((CHUNKS, pl.cdiv(width, WIDTH))), pltpu.SemaphoreType.DMA((CHUNKS, pl.cdiv(width, WIDTH))),
            pltpu.SemaphoreType.DMA((8,)), pltpu.SemaphoreType.DMA((4,)),
            pltpu.SemaphoreType.DMA((4,)), pltpu.SemaphoreType.DMA((4,)),
            pltpu.SemaphoreType.DMA((16,)),
        ],
        compiler_params=pltpu.CompilerParams(collective_id=0, has_side_effects=True, vmem_limit_bytes=60 << 20),
        cost_estimate=pl.CostEstimate(flops=10**10, bytes_accessed=40_000_000, transcendentals=2_000_000),
        name="encode",
    )(start, kept, w_in, w_out, proj, patches, gain, b_in, b_out, text, norm, qw, kw, vw, qb, vb, cos, sin)


def per_device(
    patches,
    fc_gain,
    fc_in,
    fc_in_bias,
    fc_out,
    fc_out_bias,
    proj_weight,
    text_embed,
    frame_start,
    frame_count,
    segment_ids,
    norm_gain,
    query_weight,
    query_bias,
    key_weight,
    value_weight,
    value_bias,
):
    shard_id = lax.axis_index("seq")
    shard_rows = text_embed.shape[0]
    head_size = key_weight.shape[1]
    group_size = query_weight.shape[1] // head_size

    local_slots = jnp.arange(shard_rows, dtype=jnp.int32)
    positions = shard_id * shard_rows + local_slots
    half_dim = head_size // 2
    inv_rates = jnp.exp(
        jnp.arange(half_dim, dtype=jnp.float32) * (-2.0 * math.log(rope_base) / head_size)
    )
    angles = positions.astype(jnp.float32)[:, None] * inv_rates[None, :]
    cosine, sine = jnp.cos(angles), jnp.sin(angles)
    queries, stacked = encode(
        frame_start, frame_count, fc_in[0], fc_out[0].T, proj_weight, patches[0],
        fc_gain, fc_in_bias, fc_out_bias, text_embed,
        norm_gain, query_weight, key_weight, value_weight, query_bias[None], value_bias[None],
        jnp.concatenate([cosine, cosine], axis=1), jnp.concatenate([-sine, sine], axis=1),
    )
    attended = attend(queries, stacked, segment_ids, shard_id, shard_rows)
    attended = attended.reshape(group_size, shard_rows, head_size).transpose(1, 0, 2)
    return attended.reshape(shard_rows, group_size * head_size)


def solution(mesh):
    return jax.shard_map(
        per_device,
        mesh=mesh,
        in_specs=(
            P("seq", None, None),
            P("section", None),
            P("section", "seq", None),
            P("section", None),
            P("section", None, "seq"),
            P("section", None),
            P("seq", None),
            P("seq", None),
            P(),
            P(),
            P(),
            P(),
            P(None, "section"),
            P("section"),
            P(None, "section"),
            P(None, "section"),
            P("section"),
        ),
        out_specs=P("seq", "section"),
        check_vma=False,
    )
```

```python
import functools
import math

import jax
import jax.numpy as jnp
from jax import lax
from jax.experimental import pallas as pl
from jax.experimental.pallas import tpu as pltpu
from jax.sharding import PartitionSpec as P

NZ, NX, NC = 8, 4, 2


def seq_id(z, x, c):
    return lax.rem(z + NZ, NZ) * (NX * NC) + lax.rem(x + NX, NX) * NC + c


class Ring:
    def __init__(self, send_sem, recv_sem):
        self.send_sem, self.recv_sem, self.used, self.live = send_sem, recv_sem, 0, []

    def copy(self, sent, got, target, into=None):
        n = self.used
        self.used += 1
        to = {"seq": target} if not isinstance(target, dict) else target
        sems = dict(send_sem=self.send_sem.at[n], recv_sem=self.recv_sem.at[n])
        make = functools.partial(
            pltpu.make_async_remote_copy, device_id=to, device_id_type=pl.DeviceIdType.MESH, **sems)
        out = make(src_ref=sent, dst_ref=sent if into is None else into)
        into = make(src_ref=got, dst_ref=got)
        self.live.append(out)
        return out, into

    def finish(self):
        for out in self.live:
            out.wait_send()


def greet(targets):
    barrier = pltpu.get_barrier_semaphore()
    for t in targets:
        t = {"seq": t} if not isinstance(t, dict) else t
        pl.semaphore_signal(barrier, inc=1, device_id=t, device_id_type=pl.DeviceIdType.MESH)
    return lambda: pl.semaphore_wait(barrier, len(targets))


def torus_gather(ring, me, a_one, a_many, b_one, b_many, b_like_a=False):
    z, x, c = me
    s = 1 - 2 * c
    zm, zo = seq_id(z + s, x, c), seq_id(z - s, x, c)
    xm, xo = seq_id(z, x + s, c), seq_id(z, x - s, c)
    mate = seq_id(z, x, 1 - c)
    zw = lambda k: lax.rem(z - k * s + 2 * NZ, NZ)
    xw = lambda k: lax.rem(x - k * s + 2 * NX, NX)
    one = {"a": lambda dx, dz: a_one(zw(dz), xw(dx)), "b": lambda dx, dz: b_one(zw(dz), xw(dx))}
    dxs, dzs = (0, 1, -1, 2), (0, 1, -1, 2, -2, 3, -3, 4)
    keys = sorted(
        ((kind, dx, dz) for kind in "ab" for dx in dxs for dz in dzs),
        key=lambda k: (abs(k[1]) + abs(k[2]), k[2 if k[0] == "a" else 1] != 0))
    toward = lambda d: d - 1 if d > 0 else d + 1
    copies, after = {}, {key: [] for key in keys}
    for key in keys:
        kind, dx, dz = key
        along_z = dz != 0 and (kind == "a" or dx == 0)
        if dx == dz == 0:
            continue
        source = (dx, toward(dz)) if along_z else (toward(dx), dz)
        target = (zm if dz > 0 else zo) if along_z else (xm if dx > 0 else xo)
        copies[key] = [ring.copy(sent, got, target) for sent, got in zip(one[kind](*source), one[kind](dx, dz))]
        after[(kind, *source)] += copies[key]
    am = {d: ring.copy(a_many(zw(d), c), a_many(zw(-d), 1 - c), mate) for d in dzs}
    bw, bds, late = (zw, dzs, 2) if b_like_a else (xw, dxs, 4)
    bm = {d: ring.copy(b_many(bw(d), c), b_many(bw(-d), 1 - c), mate) for d in bds}
    stages = []
    for t in range(7):
        stage = []
        for key in keys:
            if abs(key[1]) + abs(key[2]) == t:
                if t:
                    stage += [into.wait_recv for _, into in copies[key]]
                stage += [out.start for out, _ in after[key]]
        stage += [am[d][0].start for d in dzs if abs(d) + 2 == t]
        stage += [bm[d][0].start for d in bds if abs(d) + late == t]
        stages.append(stage)
    if b_like_a:
        return stages, {d: (zw(-d), [am[d][1].wait_recv, bm[d][1].wait_recv]) for d in dzs}
    return stages + [[pair[1].wait_recv for pair in (*am.values(), *bm.values())]]


def run(stage):
    for step in stage:
        step()


GATHER_COPIES = 31 + 31 + 8 + 8


def attend_kernel(
    kv_ref, q_hbm, qseg_ref, kseg_ref, o_ref,
    q_ref, a_ref, b_ref, top_ref, total_ref, acc_ref, send_sem, recv_sem, own_sem,
):
    me_seq = lax.axis_index("seq")
    z, x, c = me_seq // (NX * NC), lax.rem(me_seq // NC, NX), lax.rem(me_seq, NC)
    greeted = greet([seq_id(z + 1, x, c), seq_id(z - 1, x, c), seq_id(z, x + 1, c), seq_id(z, x - 1, c), seq_id(z, x, 1 - c)])
    half = kv_ref.shape[0] // 2
    mine = [
        pltpu.make_async_copy(kv_ref.at[pl.ds(0, half)], a_ref.at[z, x, c], own_sem.at[0]),
        pltpu.make_async_copy(kv_ref.at[pl.ds(half, half)], b_ref.at[z, x, c], own_sem.at[1]),
    ]
    for copy in mine:
        copy.start()
    queries = pltpu.make_async_copy(q_hbm, q_ref, own_sem.at[2])
    queries.start()
    greeted()
    for copy in mine:
        copy.wait()
    ring = Ring(send_sem, recv_sem)
    stages, arrivals = torus_gather(
        ring, (z, x, c),
        lambda zz, xx: (a_ref.at[zz, xx, c],), lambda zz, cc: a_ref.at[zz, :, cc],
        lambda zz, xx: (b_ref.at[zz, xx, c],), lambda zz, cc: b_ref.at[zz, :, cc], b_like_a=True)

    rows, head = q_ref.shape
    queries.wait()
    q = q_ref[...]
    qseg = qseg_ref[...]
    scale = math.log2(math.e) / math.sqrt(head)

    def visit(zz, cc, first):
        kv = [ref[zz, :, cc].reshape(NX * half, 2 * head) for ref in (a_ref, b_ref)]
        allowed = [kseg_ref[zz, cc, n : n + 1] == qseg for n in range(2)]
        if first:
            row = lax.broadcasted_iota(jnp.int32, (rows, 1), 0) & 127
            qpos = row + lax.rem(me_seq, NX * NC) * 128
            col = lax.broadcasted_iota(jnp.int32, (1, NX * half), 1)
            kpos = (col >> 6) * 256 + cc * 128 + (col & 63)
            allowed = [ok & (kpos + n * half <= qpos) for n, ok in enumerate(allowed)]
        scores = [
            lax.dot_general(q, one[:, :head], (((1,), (1,)), ((), ())), preferred_element_type=jnp.float32)
            for one in kv
        ]
        scores = [jnp.where(ok, s * scale, -1e30) for s, ok in zip(scores, allowed)]
        top = jnp.max(jnp.maximum(*scores), axis=1, keepdims=True)
        if not (first and cc is c):
            top = jnp.maximum(top_ref[...], top)
        weights = [jnp.exp2(s - top) for s in scores]
        total = jnp.sum(weights[0] + weights[1], axis=1, keepdims=True)
        acc = sum(
            jnp.dot(w.astype(jnp.bfloat16), one[:, head:], preferred_element_type=jnp.float32)
            for w, one in zip(weights, kv))
        if not (first and cc is c):
            keep = jnp.exp2(top_ref[...] - top)
            total += total_ref[...] * keep
            acc += acc_ref[...] * keep
        top_ref[...], total_ref[...], acc_ref[...] = top, total, acc

    def look_at(d, cc):
        source, waits = arrivals[d]
        if cc is not c:
            run(waits)
        if d == 0:
            visit(source, cc, True)
        else:
            @pl.when(source < z)
            def _():
                visit(source, cc, False)

    other = 1 - c
    ds = (0, 1, -1, 2, -2, 3, -3, 4)
    for t, stage in enumerate(stages):
        run(stage)
        for d in ds:
            if abs(d) + 3 == t:
                look_at(d, other)
        for d in ds:
            if abs(d) + 2 == t:
                look_at(-d if d != 4 else 4, c)
    look_at(4, other)
    o_ref[...] = (acc_ref[...] / total_ref[...]).astype(o_ref.dtype)
    ring.finish()


def attend(q, kv, segment_ids, shard, rows):
    half = rows // 2
    kseg = segment_ids.reshape(NZ, NX, NC, 2, half).transpose(0, 2, 3, 1, 4).reshape(NZ, NC, 2, NX * half)
    own = lax.dynamic_slice_in_dim(segment_ids, shard * rows, rows, 0)
    qseg = jnp.tile(own, q.shape[0] // rows)[:, None]
    whole = pl.BlockSpec(memory_space=pltpu.VMEM)
    blocks = pltpu.VMEM((NZ, NX, NC, half, kv.shape[1]), kv.dtype)
    count = q.shape[0]
    return pl.pallas_call(
        attend_kernel,
        out_shape=jax.ShapeDtypeStruct(q.shape, jnp.bfloat16),
        in_specs=[pl.BlockSpec(memory_space=pl.ANY)] * 2 + [whole] * 2,
        out_specs=whole,
        scratch_shapes=[
            pltpu.VMEM(q.shape, q.dtype), blocks, blocks,
            pltpu.VMEM((count, 1), jnp.float32), pltpu.VMEM((count, 1), jnp.float32), pltpu.VMEM(q.shape, jnp.float32),
            pltpu.SemaphoreType.DMA((GATHER_COPIES,)),
            pltpu.SemaphoreType.DMA((GATHER_COPIES,)),
            pltpu.SemaphoreType.DMA((3,)),
        ],
        compiler_params=pltpu.CompilerParams(collective_id=1, has_side_effects=True, vmem_limit_bytes=48 << 20),
        cost_estimate=pl.CostEstimate(flops=2 * 10**9, bytes_accessed=40_000_000, transcendentals=4_000_000),
        name="attend",
    )(kv, q, qseg, kseg)


CHUNKS, CHUNK, LAST = 8, 96, 64
HEAD_START, EVERY = 2, 2
WIDTH = 256
SPLIT = 112
ENC_COPIES = 14 + 2 * (3 * 31 + 12) + 8
layer_eps = 1e-06
rms_eps = 1e-06
rope_base = 1000000.0


def encoder_kernel(
    start_ref, count_ref, in_ref, out_ref, proj_ref, patches_ref, gain_ref, bin_ref, bout_ref, text_hbm,
    norm_ref, qw_hbm, kw_hbm, vw_hbm, qb_ref, vb_ref, cos_ref, sin_ref,
    q_ref, kv_ref,
    mixed_ref, qkv_ref,
    w_ref, p_ref, select_ref, frame_ref, text_ref, rec_w, rec_p, win, wout, extra, pa, pb, inflow, outflow, passed, vision,
    send_sem, recv_sem, chunk_send, chunk_recv, cast_send, cast_recv, over_send, over_recv, local_sem,
):
    me_seq, section = lax.axis_index("seq"), lax.axis_index("section")
    z, x, c = me_seq // (NX * NC), lax.rem(me_seq // NC, NX), lax.rem(me_seq, NC)
    j = lax.rem(me_seq, NX * NC)
    last = section == 3
    up, down = lax.rem(section + 1, 4), lax.rem(section + 3, 4)
    shards = NZ * NX * NC
    ahead, behind = lax.rem(me_seq + 1, shards), lax.rem(me_seq + shards - 1, shards)
    others = [lax.rem(j + k, 8) for k in range(8)]
    sources = [lax.rem(j + 8 - k, 8) for k in range(8)]
    member = lambda k: z * (NX * NC) + k

    greeted = greet(
        [member(k) for k in others[1:]]
        + [seq_id(z + 1, x, c), seq_id(z - 1, x, c), ahead, behind, {"section": up}, {"section": down}]
    )
    frame = pltpu.make_async_copy(patches_ref, frame_ref, local_sem.at[2])
    text = pltpu.make_async_copy(text_hbm, text_ref, local_sem.at[11])
    heads = qw_hbm.shape[1]
    head = kw_hbm.shape[1]
    loads = [text] + [
        pltpu.make_async_copy(ref, qkv_ref.at[:, pl.ds(at, ref.shape[1])], local_sem.at[12 + n])
        for n, (ref, at) in enumerate(((qw_hbm, 0), (kw_hbm, heads), (vw_hbm, heads + head)))
    ]
    for copy in loads:
        copy.start()

    @pl.when(section == 0)
    def _():
        frame.start()

    inflow[CHUNKS - 1, LAST:] = jnp.zeros((CHUNK - LAST, inflow.shape[2]), inflow.dtype)
    depth = in_ref.shape[0]
    w_ref[:, 16:, :] = jnp.zeros((8, 16, w_ref.shape[2]), w_ref.dtype)
    p_ref[:, 16:, :] = jnp.zeros((8, 16, p_ref.shape[2]), p_ref.dtype)
    p_ref[7] = jnp.zeros(p_ref.shape[1:], p_ref.dtype)
    for k in range(8):
        w_ref[k, :depth, :256] = in_ref[:, 256 * k : 256 * k + 256]
        w_ref[k, :depth, 256:512] = out_ref[:, 256 * k : 256 * k + 256]
        w_ref[k, :depth, 512:] = (out_ref if k % 2 else in_ref)[:, 2048:]
        if k < 7:
            p_ref[k, :depth] = proj_ref[:, 512 * k : 512 * k + 512]
    own = [
        pltpu.make_async_copy(w_ref.at[j], rec_w.at[j], local_sem.at[0]),
        pltpu.make_async_copy(p_ref.at[j], rec_p.at[j], local_sem.at[1]),
    ]
    rows = win.shape[3]
    at = lax.broadcasted_iota(jnp.int32, (rows, 256), 0)
    slot = lax.broadcasted_iota(jnp.int32, (rows, 256), 1)
    inner = slot & 31
    pick = jnp.where((inner < depth) & (at == depth * (slot >> 5) + inner), 1.0, 0.0).astype(jnp.bfloat16)

    greeted()
    ring = Ring(send_sem, recv_sem)
    spread_w = [ring.copy(w_ref.at[others[k]], rec_w.at[sources[k]], member(others[k]), rec_w.at[j]) for k in range(1, 8)]
    spread_p = [ring.copy(p_ref.at[others[k]], rec_p.at[sources[k]], member(others[k]), rec_p.at[j]) for k in range(1, 8)]
    for out, _ in spread_w:
        out.start()
    for copy in own:
        copy.start()
    for copy in own:
        copy.wait()
    for _, into in spread_w:
        into.wait_recv()
    block = jnp.dot(pick, rec_w[...].reshape(-1, rec_w.shape[2]), preferred_element_type=jnp.float32)
    block = block.astype(jnp.bfloat16)
    wout[x, c, z] = block[:, 256:512]
    win[x, c, z] = block[:, :256]
    extra[c, z] = block[:, 512:]

    def views(a, b):
        return (
            lambda zz, xx: (a.at[xx, c, zz, pl.ds(0, SPLIT)],),
            lambda zz, cc: a.at[:, cc, zz],
            lambda zz, xx: (b.at[xx, c, zz], a.at[xx, c, zz, pl.ds(SPLIT, rows - SPLIT)]),
            lambda xx, cc: b.at[xx, cc])

    stages = torus_gather(ring, (z, x, c), *views(win, wout))
    s = 1 - 2 * c
    zw = lambda k: lax.rem(z + k + 2 * NZ, NZ)
    zm, zo = seq_id(z + s, x, c), seq_id(z - s, x, c)
    ez_m = [ring.copy(extra.at[c, zw(-k * s)], extra.at[c, zw(-(k + 1) * s)], zm) for k in range(4)]
    ez_o = [ring.copy(extra.at[c, zw(k * s)], extra.at[c, zw((k + 1) * s)], zo) for k in range(3)]
    e_mate = ring.copy(extra.at[c], extra.at[1 - c], seq_id(z, x, 1 - c))
    for n, stage in enumerate(stages):
        if n == 7:
            e_mate[0].start()
        run(stage)
        if n == 2:
            ez_m[0][0].start()
            ez_o[0][0].start()
        if 3 <= n < 7:
            ez_m[n - 3][1].wait_recv()
            if n < 6:
                ez_m[n - 2][0].start()
                ez_o[n - 3][1].wait_recv()
            if n < 5:
                ez_o[n - 2][0].start()
    e_mate[1].wait_recv()
    for out, _ in spread_p:
        out.start()

    def lay_out_p():
        for _, into in spread_p:
            into.wait_recv()
        block = jnp.dot(pick, rec_p[...].reshape(-1, rec_p.shape[2]), preferred_element_type=jnp.float32)
        block = block.astype(jnp.bfloat16)
        pa[x, c, z] = block[:, :256]
        pb[x, c, z] = block[:, 256:]

    p_stages = [[lay_out_p]] + torus_gather(ring, (z, x, c), *views(pa, pb))

    @pl.when(section == 0)
    def _():
        frame.wait()
        full = frame_ref.shape[0] // CHUNK
        for i in range(full):
            inflow[i] = frame_ref[CHUNK * i : CHUNK * i + CHUNK]
        inflow[full] = jnp.zeros((CHUNK, frame_ref.shape[1]), inflow.dtype)
        inflow[full, : frame_ref.shape[0] - CHUNK * full] = frame_ref[CHUNK * full :]

    for n in range(3 * HEAD_START):
        @pl.when(n < HEAD_START * section)
        def _():
            run(p_stages[n])

    count = text_ref.shape[0]
    first, kept = start_ref[me_seq], count_ref[me_seq]

    @pl.when(last)
    def _():
        shape = select_ref.shape
        token = lax.broadcasted_iota(jnp.int32, (shape[0], 1), 0) + (me_seq * count - first)
        patch = lax.broadcasted_iota(jnp.int32, (1, shape[1]), 1)
        down = (patch * 607) >> 14
        across = patch - 27 * down
        cell = jnp.where(patch < 729, (down >> 1) * 14 + (across >> 1), -1)
        share = jnp.where(down == 26, 1.0, 0.5) * jnp.where(across == 26, 1.0, 0.5)
        token = jnp.where((token >= 0) & (token < kept), token, -2)
        select_ref[...] = jnp.where(token == cell, share, 0.0).astype(jnp.bfloat16)

    def chunk_copy(i, size):
        return pltpu.make_async_remote_copy(
            src_ref=outflow.at[i, pl.ds(0, size)], dst_ref=inflow.at[i, pl.ds(0, size)],
            send_sem=chunk_send.at[i], recv_sem=chunk_recv.at[i],
            device_id={"section": up}, device_id_type=pl.DeviceIdType.MESH)

    def one_chunk(i, nothing):
        @pl.when((section > 0) & (i < CHUNKS - 1))
        def _():
            chunk_copy(i, CHUNK).wait_recv()

        @pl.when((section > 0) & (i == CHUNKS - 1))
        def _():
            chunk_copy(i, LAST).wait_recv()

        widened = inflow[i].astype(jnp.float32)
        center = widened - jnp.mean(widened, axis=1, keepdims=True)
        spread = jnp.mean(center * center, axis=1, keepdims=True)
        normed = (center * lax.rsqrt(spread + layer_eps) * gain_ref[...]).astype(jnp.bfloat16)

        def hidden(w_in, b_in):
            v = jnp.dot(normed, w_in, preferred_element_type=jnp.float32) + b_in
            return jax.nn.gelu(v, approximate=True).astype(jnp.bfloat16)

        flat = lambda ref, k: ref[k // 2, k % 2].reshape(8 * rows, 256)
        parts = [hidden(flat(win, k), bin_ref[:, 256 * k : 256 * k + 256]) for k in range(8)]
        parts.append(hidden(extra[0].reshape(8 * rows, 128), bin_ref[:, 2048:]))
        for at in range(0, 8 * rows, WIDTH):
            to = min(at + WIDTH, 8 * rows)
            out = widened[:, at:to] + bout_ref[:, at:to]
            for k in range(9):
                w_out = flat(wout, k) if k < 8 else extra[1].reshape(8 * rows, 128)
                out += lax.dot_general(
                    parts[k], w_out[at:to], (((1,), (1,)), ((), ())), preferred_element_type=jnp.float32)
            outflow[i, :, at:to] = out.astype(jnp.bfloat16)

        @pl.when(jnp.logical_not(last) & (i < CHUNKS - 1))
        def _():
            chunk_copy(i, CHUNK).start()

        @pl.when(jnp.logical_not(last) & (i == CHUNKS - 1))
        def _():
            chunk_copy(i, LAST).start()

        for n, stage in enumerate(p_stages):
            @pl.when((i == EVERY * (n - HEAD_START * section)) & (section > 0))
            def _():
                run(stage)

        return nothing

    lax.fori_loop(0, CHUNKS, one_chunk, 0)

    for n, stage in enumerate(p_stages):
        @pl.when((EVERY * (n - HEAD_START * section) >= CHUNKS) | (section == 0))
        def _():
            run(stage)

    @pl.when(jnp.logical_not(last))
    def _():
        for i in range(CHUNKS):
            chunk_copy(i, CHUNK if i < CHUNKS - 1 else LAST).wait_send()

    over = lambda h: pltpu.make_async_remote_copy(
        src_ref=passed.at[0, h], dst_ref=passed.at[1, h], send_sem=over_send.at[h], recv_sem=over_recv.at[h],
        device_id={"seq": ahead}, device_id_type=pl.DeviceIdType.MESH)
    parts = vision.shape[0]
    order, handed = (0, 3, 1, 2), {0: (0, 1), 2: (3, 2)}
    cast = lambda h, n, to: pltpu.make_async_remote_copy(
        src_ref=vision.at[h], dst_ref=vision.at[h], send_sem=cast_send.at[n], recv_sem=cast_recv.at[h],
        device_id={"section": to}, device_id_type=pl.DeviceIdType.MESH)

    @pl.when(last)
    def _():
        encoded = outflow[...].reshape(CHUNKS * CHUNK, outflow.shape[2])
        out = jnp.dot(select_ref[count:], encoded, preferred_element_type=jnp.float32)
        passed[0] = out.astype(jnp.bfloat16).reshape(vision.shape)
        for h in order:
            over(h).start()
        mine = jnp.dot(select_ref[:count], encoded, preferred_element_type=jnp.float32)
        mine = mine.reshape(vision.shape)
        for h in order:
            over(h).wait_recv()
            other = jnp.where(me_seq > 0, passed[1, h].astype(jnp.float32), 0.0)
            vision[h] = (mine[h] + other).astype(jnp.bfloat16)
            cast(h, h, 0).start()
            cast(h, parts + h, 2).start()
        for h in order:
            over(h).wait_send()
            cast(h, h, 0).wait_send()
            cast(h, parts + h, 2).wait_send()

    for me, mine in handed.items():
        @pl.when(section == me)
        def _():
            for h in order:
                cast(h, h, 1).wait_recv()
                if h in mine:
                    cast(h, h, 1).start()
            for h in mine:
                cast(h, h, 1).wait_send()

    @pl.when(section == 1)
    def _():
        for h in range(parts):
            cast(h, h, 1).wait_recv()

    tokens = vision[...].reshape(count, vision.shape[2])
    for copy in loads:
        copy.wait()
    slots = lax.broadcasted_iota(jnp.int32, (count, 1), 0) + me_seq * count
    before = jnp.maximum(me_seq - 1, 0)
    prior = slots - start_ref[before]
    valid = (slots >= first) & (slots < first + kept)
    valid = valid | ((me_seq > 0) & (prior >= 0) & (prior < count_ref[before]))
    squares = jnp.zeros((count, 1), jnp.float32)
    for k in range(7):
        for n, ref in enumerate((pa, pb)):
            out = jnp.dot(tokens, ref[k // 2, k % 2].reshape(8 * rows, 256), preferred_element_type=jnp.float32)
            at = 512 * k + 256 * n
            out = jnp.where(valid, out.astype(jnp.bfloat16), text_ref[:, at : at + 256])
            mixed_ref[:, at : at + 256] = out
            out = out.astype(jnp.float32)
            squares += jnp.sum(out * out, axis=1, keepdims=True)
    factor = lax.rsqrt(squares / mixed_ref.shape[1] + rms_eps)
    normed = (mixed_ref[...].astype(jnp.float32) * factor * norm_ref[...]).astype(jnp.bfloat16)
    rope = lambda u: u * cos_ref[...] + pltpu.roll(u, head // 2, 1) * sin_ref[...]
    for n in range(0, heads, 2 * head):
        two = jnp.dot(normed, qkv_ref[:, n : n + 2 * head], preferred_element_type=jnp.float32)
        two = two + qb_ref[:, n : n + 2 * head]
        for i in range(2):
            at = (n // head + i) * count
            q_ref[at : at + count] = rope(two[:, i * head : (i + 1) * head]).astype(jnp.bfloat16)
    two = jnp.dot(normed, qkv_ref[:, heads:], preferred_element_type=jnp.float32)
    kv_ref[:, :head] = rope(two[:, :head]).astype(jnp.bfloat16)
    kv_ref[:, head:] = (two[:, head:] + vb_ref[...]).astype(jnp.bfloat16)
    ring.finish()


def encode(start, kept, w_in, w_out, proj, patches, gain, b_in, b_out, text, norm, qw, kw, vw, qb, vb, cos, sin):
    rows, width = 8 * w_in.shape[0], patches.shape[1]
    whole = pl.BlockSpec(memory_space=pltpu.VMEM)
    scalars = pl.BlockSpec(memory_space=pltpu.SMEM)
    away = pl.BlockSpec(memory_space=pl.ANY)
    bf = jnp.bfloat16
    big = pltpu.VMEM((NX, NC, NZ, rows, 256), bf)
    spread = [pltpu.VMEM((8, 32, 640), bf), pltpu.VMEM((8, 32, 512), bf)]
    return pl.pallas_call(
        encoder_kernel,
        out_shape=(
            jax.ShapeDtypeStruct((text.shape[0] * (qw.shape[1] // kw.shape[1]), kw.shape[1]), bf),
            jax.ShapeDtypeStruct((text.shape[0], 2 * kw.shape[1]), bf),
        ),
        in_specs=[scalars, scalars, whole, whole, whole, away, whole, whole, whole, away]
        + [whole, away, away, away] + [whole] * 4,
        out_specs=(whole, whole),
        scratch_shapes=[
            pltpu.VMEM(text.shape, bf), pltpu.VMEM((text.shape[1], qw.shape[1] + 2 * kw.shape[1]), bf),
            *spread, pltpu.VMEM((2 * text.shape[0], CHUNKS * CHUNK), bf),
            pltpu.VMEM(patches.shape, bf), pltpu.VMEM(text.shape, bf), *spread,
            big, big, pltpu.VMEM((NC, NZ, rows, 128), bf), big, big,
            pltpu.VMEM((CHUNKS, CHUNK, width), bf), pltpu.VMEM((CHUNKS, CHUNK, width), bf),
            pltpu.VMEM((2, 4, text.shape[0] // 4, width), bf), pltpu.VMEM((4, text.shape[0] // 4, width), bf),
            pltpu.SemaphoreType.DMA((ENC_COPIES,)), pltpu.SemaphoreType.DMA((ENC_COPIES,)),
            pltpu.SemaphoreType.DMA((CHUNKS,)), pltpu.SemaphoreType.DMA((CHUNKS,)),
            pltpu.SemaphoreType.DMA((8,)), pltpu.SemaphoreType.DMA((4,)),
            pltpu.SemaphoreType.DMA((4,)), pltpu.SemaphoreType.DMA((4,)),
            pltpu.SemaphoreType.DMA((16,)),
        ],
        compiler_params=pltpu.CompilerParams(collective_id=0, has_side_effects=True, vmem_limit_bytes=60 << 20),
        cost_estimate=pl.CostEstimate(flops=10**10, bytes_accessed=40_000_000, transcendentals=2_000_000),
        name="encode",
    )(start, kept, w_in, w_out, proj, patches, gain, b_in, b_out, text, norm, qw, kw, vw, qb, vb, cos, sin)


def per_device(
    patches,
    fc_gain,
    fc_in,
    fc_in_bias,
    fc_out,
    fc_out_bias,
    proj_weight,
    text_embed,
    frame_start,
    frame_count,
    segment_ids,
    norm_gain,
    query_weight,
    query_bias,
    key_weight,
    value_weight,
    value_bias,
):
    shard_id = lax.axis_index("seq")
    shard_rows = text_embed.shape[0]
    head_size = key_weight.shape[1]
    group_size = query_weight.shape[1] // head_size

    local_slots = jnp.arange(shard_rows, dtype=jnp.int32)
    positions = shard_id * shard_rows + local_slots
    half_dim = head_size // 2
    inv_rates = jnp.exp(
        jnp.arange(half_dim, dtype=jnp.float32) * (-2.0 * math.log(rope_base) / head_size)
    )
    angles = positions.astype(jnp.float32)[:, None] * inv_rates[None, :]
    cosine, sine = jnp.cos(angles), jnp.sin(angles)
    queries, stacked = encode(
        frame_start, frame_count, fc_in[0], fc_out[0].T, proj_weight, patches[0],
        fc_gain, fc_in_bias, fc_out_bias, text_embed,
        norm_gain, query_weight, key_weight, value_weight, query_bias[None], value_bias[None],
        jnp.concatenate([cosine, cosine], axis=1), jnp.concatenate([-sine, sine], axis=1),
    )
    attended = attend(queries, stacked, segment_ids, shard_id, shard_rows)
    attended = attended.reshape(group_size, shard_rows, head_size).transpose(1, 0, 2)
    return attended.reshape(shard_rows, group_size * head_size)


def solution(mesh):
    return jax.shard_map(
        per_device,
        mesh=mesh,
        in_specs=(
            P("seq", None, None),
            P("section", None),
            P("section", "seq", None),
            P("section", None),
            P("section", None, "seq"),
            P("section", None),
            P("seq", None),
            P("seq", None),
            P(),
            P(),
            P(),
            P(),
            P(None, "section"),
            P("section"),
            P(None, "section"),
            P(None, "section"),
            P("section"),
        ),
        out_specs=P("seq", "section"),
        check_vma=False,
    )
```
